256 devices in a mesh: section: 8 (over x_hi, y), shard: 32 (over z, x_lo, core).
Axes of the slice: x: 4 (x_hi: 2, x_lo: 2; x = x_hi * 2 + x_lo), y: 4, z: 8, core: 2. Of those that a mesh axis runs over, the one named last changes fastest.
Arguments:
- activations: bfloat16 [8, 3072, 4096], P('section', 'shard'), may hold values from -30 to 30, as said below
- top_grad: bfloat16 [3072, 4096], P('shard'), may hold values from -6 to 6
- loss_mask: int32 [3072], P('shard'), may hold values 0 or 1
- norm_gain: float32 [8, 4096], P('section'), may hold values from 0.5 to 1.5
- value_weight: bfloat16 [8, 4096, 1024], P('section', 'shard'), may hold values from -0.046875 to 0.046875
- output_weight: bfloat16 [8, 1024, 4096], P('section', None, 'shard'), may hold values from -0.09375 to 0.09375
- value_proj: bfloat16 [8, 1024, 64], P('section'), may hold values from -0.1875 to 0.1875
- grad_proj: bfloat16 [8, 4096, 64], P('section'), may hold values from -0.09375 to 0.09375
- store: float32 [8, 4096, 4096], P('section', 'shard'), may hold values from -0.024 to 0.024
Outputs:
- scores: float32 [32, 4096], P('section', 'shard')
The draws below stay inside these ranges and needn't reach their ends.
Inputs may be any that keep to these rules, and one draw needn't show every extreme that they name: activations of order one per token.
All inputs are finite; a program needn't handle non-finite values. No bound on the sum of `loss_mask` on one device may be relied on, other than what follows from the above.
Results may differ from the reference program's by a relative error of at most 0.007.
Values may be sent and summed in bfloat16 or wider, within the bound.
A program may use at most 128 MiB of HBM per device.

```python
import jax
import jax.numpy as jnp
from jax import lax

D = 4096
KV = 1024
PROJ = 64
LEN = 96
LAYERS = 8
GENS = 32
TOKENS = 3072
STORE = 4096


def draw_activations(key, part):
    key_base, key_column, key_row = jax.random.split(key, 3)
    grid_shape = (LAYERS, TOKENS, D)
    sample_base = jnp.clip(jax.random.normal(key_base, grid_shape, jnp.float32), -5.0, 5.0)
    column_scale = jnp.exp(jax.random.uniform(key_column, (LAYERS, 1, D), jnp.float32, -1.1, 1.1))
    row_scale = jnp.exp(jax.random.uniform(key_row, (LAYERS, TOKENS, 1), jnp.float32, -0.69, 0.69))
    return (sample_base * column_scale * row_scale).astype(jnp.bfloat16)


def with_ends(values, own_key, smallest, largest):
    extent = values.shape
    spot = [jax.random.randint(jax.random.fold_in(own_key, axis), (), 0, extent[axis]) for axis in range(len(extent))]
    values = values.at[tuple(spot)].set(smallest)
    longest = extent.index(max(extent))
    spot[longest] = (spot[longest] + 1) % extent[longest]
    return values.at[tuple(spot)].set(largest)


def steps_of(stream_key, extent, cuts, smallest, high):
    def one(axis_at, shards_of):
        heights = jax.random.uniform(jax.random.fold_in(jax.random.fold_in(stream_key, 6), axis_at), (shards_of,), jnp.float32, smallest / len(cuts), high / len(cuts))
        return jnp.repeat(jnp.exp(heights), extent[axis_at] // shards_of).reshape((-1,) + (1,) * (len(extent) - axis_at - 1))

    factor_of = one(*cuts[0])
    for cut in cuts[1:]:
        factor_of = factor_of * one(*cut)
    return factor_of


def bell_draw(rng, shape, width, reach, pieces=(), held_as=jnp.bfloat16):
    result = width * jax.random.normal(rng, shape, jnp.float32)
    if pieces:
        result = result * steps_of(rng, shape, pieces, -0.22, 0.18)
    return jnp.clip(result, -reach, reach).astype(held_as)


def setup_inputs(seed: int = 0) -> dict:
    seeds = jax.random.split(jax.random.key(seed), 10)
    activations = draw_activations(jax.random.fold_in(seeds[9], 71), 0)
    top_grad = bell_draw(seeds[1], (TOKENS, D), 1.0, 6.0, ((0, 32),))
    loss_mask = with_ends((jax.random.randint(seeds[2], (TOKENS,), 0, 4) < 3).astype(jnp.int32), jax.random.fold_in(seeds[2], 1), 0, 1)
    norm_gain = jnp.clip(1.0 + 0.1 * jax.random.normal(seeds[3], (LAYERS, D), jnp.float32), 0.5, 1.5)
    value_weight = bell_draw(seeds[4], (LAYERS, D, KV), (4 * D) ** -0.5, 0.046875, ((0, 8), (1, 32)))
    output_weight = bell_draw(seeds[5], (LAYERS, KV, D), D ** -0.5, 0.09375, ((0, 8), (2, 32)))
    value_proj = bell_draw(seeds[6], (LAYERS, KV, PROJ), KV ** -0.5, 0.1875, ((0, 8),))
    grad_proj = bell_draw(seeds[7], (LAYERS, D, PROJ), D ** -0.5, 0.09375, ((0, 8),))
    store = bell_draw(seeds[8], (LAYERS, STORE, PROJ * PROJ), 0.004, 0.024, ((0, 8), (1, 32)), jnp.float32)
    return {"activations": activations, "top_grad": top_grad, "loss_mask": loss_mask, "norm_gain": norm_gain, "value_weight": value_weight, "output_weight": output_weight, "value_proj": value_proj, "grad_proj": grad_proj, "store": store}


EPSILON = 1e-05

def reference(activations, top_grad, loss_mask, norm_gain, value_weight, output_weight, value_proj, grad_proj, store):
    cotangent = (top_grad.astype(jnp.float32) * loss_mask.astype(jnp.float32)[:, None]).astype(jnp.bfloat16)
    score_total = jnp.zeros((GENS, STORE), jnp.float32)
    for layer_index in range(LAYERS - 1, -1, -1):
        hidden_in = activations[layer_index].astype(jnp.float32)
        inverse_rms = lax.rsqrt(lax.optimization_barrier(jnp.mean(hidden_in * hidden_in, axis=-1, keepdims=True)) + EPSILON)
        norm_scale = norm_gain[layer_index]
        normed = (hidden_in * inverse_rms * norm_scale).astype(jnp.bfloat16)
        value_act = jnp.dot(normed, value_weight[layer_index], preferred_element_type=jnp.float32).astype(jnp.bfloat16)
        value_low = jnp.dot(value_act, value_proj[layer_index], preferred_element_type=jnp.float32)
        grad_low = jnp.dot(cotangent, grad_proj[layer_index], preferred_element_type=jnp.float32)
        features = jnp.einsum('gta,gtb->gab', grad_low.reshape(GENS, LEN, PROJ), value_low.reshape(GENS, LEN, PROJ), precision=lax.Precision.HIGHEST).reshape(GENS, PROJ * PROJ)
        score_total = score_total + lax.dot_general(features, store[layer_index], (((1,), (1,)), ((), ())), precision=lax.Precision.HIGHEST, preferred_element_type=jnp.float32)
        if layer_index > 0:
            grad_value = lax.dot_general(cotangent, output_weight[layer_index], (((1,), (1,)), ((), ())), preferred_element_type=jnp.float32).astype(jnp.bfloat16)
            grad_normed = lax.dot_general(grad_value, value_weight[layer_index], (((1,), (1,)), ((), ())), preferred_element_type=jnp.float32)
            scaled = norm_scale * grad_normed
            correction = lax.optimization_barrier(jnp.mean(scaled * hidden_in, axis=-1, keepdims=True))
            grad_input = inverse_rms * scaled - hidden_in * (inverse_rms * inverse_rms * inverse_rms) * correction
            cotangent = (cotangent.astype(jnp.float32) + grad_input).astype(jnp.bfloat16)
    return score_total
```

```python
import jax
import jax.numpy as jnp
from jax import lax
from jax.experimental import pallas as pl
from jax.experimental.pallas import tpu as pltpu
from jax.sharding import PartitionSpec as P

LEN = 96
EPSILON = 1e-05
MESH = pl.DeviceIdType.MESH
NZ = 8
SECTIONS = 8
ROWS = 16
BLOCKS = LEN // ROWS


def chain_kernel(
    act, top, mask, gain, vt_own, ot_own, vproj, gproj,
    feat,
    wvt, wot, normed, rms, c_in, c_out, scaled, va, vlow,
    zs, zr, xs, xr, ds_, dr, cs, cr,
):
    sec = lax.axis_index("section")
    shard = lax.axis_index("shard")
    z = shard // 4
    xl = (shard // 2) % 2
    core = shard % 2
    width = act.shape[1]
    kv = wot.shape[1]
    cols = vt_own.shape[1]

    def dev(z_, x_, c_):
        return (sec, z_ * 4 + x_ * 2 + c_)

    z_next = (z + 1) % NZ
    z_prev = (z + NZ - 1) % NZ
    up = (sec + 1) % SECTIONS
    down = (sec + SECTIONS - 1) % SECTIONS
    barrier = pltpu.get_barrier_semaphore()
    peers = (
        dev(z_next, xl, core), dev(z_prev, xl, core), dev(z, 1 - xl, core), dev(z, xl, 1 - core),
        (up, shard), (down, shard),
    )
    for peer in peers:
        pl.semaphore_signal(barrier, inc=1, device_id=peer, device_id_type=MESH)
    pl.semaphore_wait(barrier, len(peers))

    def v_block(z_, x_, c_, half):
        first = pl.multiple_of((z_ * 4 + x_ * 2 + c_) * cols, cols)
        if half is None:
            return wvt.at[:, pl.ds(first, cols)]
        return wvt.at[pl.ds(half * (kv // 2), kv // 2), pl.ds(first, cols)]

    def o_block(z_, x_, c_, half):
        first = (z_ * 4 + x_ * 2 + c_) * cols
        if half is None:
            return wot.at[pl.ds(pl.multiple_of(first, cols), cols), :]
        return wot.at[pl.ds(pl.multiple_of(first + half * (cols // 2), cols // 2), cols // 2), :]

    def block(item, z_, c_, half):
        if item == 0:
            return v_block(z_, xl, c_, half)
        return o_block(z_, xl if item == 1 else 1 - xl, c_, half)

    def origin(direction, hops):
        return (z + (NZ - hops if direction == 0 else hops)) % NZ

    def z_copy(direction, k, item):
        half = None if k < 3 else direction
        zo = origin(direction, k)
        dst = block(item, zo, core, half)
        src = (vt_own if item == 0 else ot_own) if k == 0 and item < 2 else dst
        return pltpu.make_async_remote_copy(
            src_ref=src, dst_ref=dst, send_sem=zs.at[direction, k, item], recv_sem=zr.at[direction, k, item],
            device_id=dev(z_next if direction == 0 else z_prev, xl, core), device_id_type=MESH,
        )

    def z_arrival(direction, k, item):
        half = None if k < 3 else direction
        ref = block(item, origin(direction, k + 1), core, half)
        return pltpu.make_async_remote_copy(
            src_ref=ref, dst_ref=ref, send_sem=zs.at[direction, k, item], recv_sem=zr.at[direction, k, item],
            device_id=dev(z_prev if direction == 0 else z_next, xl, core), device_id_type=MESH,
        )

    def x_refs(index, x_):
        if index == 0:
            return o_block(z, x_, core, None)
        if index == 1:
            return v_block(z, x_, core, None)
        direction, k = (index - 2) // 4, (index - 2) % 4
        return v_block(origin(direction, k + 1), x_, core, None if k < 3 else direction)

    def x_copy(index):
        dst = x_refs(index, xl)
        src = (ot_own, vt_own)[index] if index < 2 else dst
        return pltpu.make_async_remote_copy(
            src_ref=src, dst_ref=dst, send_sem=xs.at[index], recv_sem=xr.at[index],
            device_id=dev(z, 1 - xl, core), device_id_type=MESH,
        )

    def x_arrival(index):
        ref = x_refs(index, 1 - xl)
        return pltpu.make_async_remote_copy(
            src_ref=ref, dst_ref=ref, send_sem=xs.at[index], recv_sem=xr.at[index],
            device_id=dev(z, 1 - xl, core), device_id_type=MESH,
        )

    def d_refs(index, c_):
        if index == 0:
            return o_block(z, xl, c_, None)
        if index == 1:
            return v_block(z, xl, c_, None)
        if index < 26:
            direction, k, item = (index - 2) // 12, (index - 2) // 3 % 4, (index - 2) % 3
            return block(item, origin(direction, k + 1), c_, None if k < 3 else direction)
        index -= 26
        if index == 0:
            return o_block(z, 1 - xl, c_, None)
        if index == 1:
            return v_block(z, 1 - xl, c_, None)
        direction, k = (index - 2) // 4, (index - 2) % 4
        return v_block(origin(direction, k + 1), 1 - xl, c_, None if k < 3 else direction)

    def d_copy(index):
        dst = d_refs(index, core)
        src = (ot_own, vt_own)[index] if index < 2 else dst
        return pltpu.make_async_remote_copy(
            src_ref=src, dst_ref=dst, send_sem=ds_.at[index], recv_sem=dr.at[index],
            device_id=dev(z, xl, 1 - core), device_id_type=MESH,
        )

    def d_arrival(index):
        ref = d_refs(index, 1 - core)
        return pltpu.make_async_remote_copy(
            src_ref=ref, dst_ref=ref, send_sem=ds_.at[index], recv_sem=dr.at[index],
            device_id=dev(z, xl, 1 - core), device_id_type=MESH,
        )

    started = []

    def start(copy):
        copy.start()
        started.append(copy)

    start(x_copy(0))
    start(x_copy(1))
    for item in (0, 1):
        for direction in (0, 1):
            start(z_copy(direction, 0, item))
    start(d_copy(0))
    start(d_copy(1))
    own = pl.ds(pl.multiple_of(shard * cols, cols), cols)
    wvt[:, own] = vt_own[...]
    wot[own, :] = ot_own[...]

    def prepare(b, carry):
        rows = pl.ds(pl.multiple_of(b * ROWS, ROWS), ROWS)
        hidden = act[rows, :].astype(jnp.float32)
        inverse = lax.rsqrt(jnp.mean(hidden * hidden, axis=-1, keepdims=True) + EPSILON)
        rms[rows, :] = jnp.broadcast_to(inverse, (ROWS, 128))
        normed[rows, :] = (hidden * inverse * gain[...]).astype(jnp.bfloat16)
        return carry

    lax.fori_loop(0, BLOCKS, prepare, 0)

    @pl.when(sec == SECTIONS - 1)
    def _():
        def masked(b, carry):
            rows = pl.ds(pl.multiple_of(b * ROWS, ROWS), ROWS)
            row_at = lax.broadcasted_iota(jnp.int32, (ROWS, LEN), 0) + b * ROWS
            col_at = lax.broadcasted_iota(jnp.int32, (ROWS, LEN), 1)
            kept = jnp.where(row_at == col_at, mask[...].astype(jnp.float32), 0.0)
            column = jnp.sum(kept, axis=-1, keepdims=True)
            c_in[b] = (top[rows, :].astype(jnp.float32) * column).astype(jnp.bfloat16)
            return carry

        lax.fori_loop(0, BLOCKS, masked, 0)

    x_arrival(0).wait_recv()
    for direction in (0, 1):
        start(z_copy(direction, 0, 2))
    start(d_copy(26))
    x_arrival(1).wait_recv()
    start(d_copy(27))
    for k in range(4):
        for item in range(3):
            for direction in (0, 1):
                z_arrival(direction, k, item).wait_recv()
                if k < 3:
                    start(z_copy(direction, k + 1, item))
                if item == 0:
                    start(x_copy(2 + direction * 4 + k))
                start(d_copy(2 + direction * 12 + k * 3 + item))
        for direction in (0, 1):
            x_arrival(2 + direction * 4 + k).wait_recv()
            start(d_copy(26 + 2 + direction * 4 + k))
    for index in range(36):
        d_arrival(index).wait_recv()

    def value_path():
        for n in range(0, kv, 256):
            part = lax.dot_general(
                normed[...], wvt[n : n + 256, :], (((1,), (1,)), ((), ())), preferred_element_type=jnp.float32
            )
            va[:, n : n + 256] = part.astype(jnp.bfloat16)
        vlow[...] = jnp.dot(va[...], vproj[...], preferred_element_type=jnp.float32)

    def c_copy(b):
        return pltpu.make_async_remote_copy(
            src_ref=c_out.at[b], dst_ref=c_in.at[b], send_sem=cs.at[b], recv_sem=cr.at[b],
            device_id=(down, shard), device_id_type=MESH,
        )

    def c_arrival(b):
        return pltpu.make_async_remote_copy(
            src_ref=c_in.at[b], dst_ref=c_in.at[b], send_sem=cs.at[b], recv_sem=cr.at[b],
            device_id=(up, shard), device_id_type=MESH,
        )

    @pl.when(sec < SECTIONS - 1)
    def _():
        value_path()

    def stage(b, carry):
        @pl.when(sec < SECTIONS - 1)
        def _():
            c_arrival(b).wait_recv()

        @pl.when(sec > 0)
        def _():
            rows = pl.ds(pl.multiple_of(b * ROWS, ROWS), ROWS)
            grad_value = jnp.dot(c_in[b], wot[...], preferred_element_type=jnp.float32).astype(jnp.bfloat16)
            total = jnp.zeros((ROWS, 1), jnp.float32)
            step = 512
            for n in range(0, width, step):
                part = jnp.dot(grad_value, wvt[:, n : n + step], preferred_element_type=jnp.float32)
                part = gain[:, n : n + step] * part
                scaled[:, n : n + step] = part
                hidden = act[rows, n : n + step].astype(jnp.float32)
                total += jnp.sum(part * hidden, axis=-1, keepdims=True)
            inverse = rms[rows, :][:, :1]
            back = (inverse * inverse * inverse) * (total / width)
            for n in range(0, width, step):
                hidden = act[rows, n : n + step].astype(jnp.float32)
                grad_input = inverse * scaled[:, n : n + step] - hidden * back
                c_out[b, :, n : n + step] = (
                    c_in[b, :, n : n + step].astype(jnp.float32) + grad_input
                ).astype(jnp.bfloat16)
            c_copy(b).start()

        return carry

    lax.fori_loop(0, BLOCKS, stage, 0)

    @pl.when(sec == SECTIONS - 1)
    def _():
        value_path()

    low = jnp.dot(
        c_in[...].reshape(LEN, width), gproj[...], preferred_element_type=jnp.float32
    )
    feat[...] = lax.dot_general(
        low, vlow[...], (((0,), (0,)), ((), ())),
        precision=lax.Precision.HIGHEST, preferred_element_type=jnp.float32,
    )
    for copy in started:
        copy.wait_send()

    @pl.when(sec > 0)
    def _():
        def sent(b, carry):
            c_copy(b).wait_send()
            return carry

        lax.fori_loop(0, BLOCKS, sent, 0)


def chain(act, top, mask, gain, vt_own, ot_own, vproj, gproj):
    tokens, width = act.shape
    kv = vt_own.shape[0]
    proj = vproj.shape[1]
    vmem = pl.BlockSpec(memory_space=pltpu.VMEM)
    dma = pltpu.SemaphoreType.DMA
    return pl.pallas_call(
        chain_kernel,
        out_shape=jax.ShapeDtypeStruct((proj, proj), jnp.float32),
        in_specs=[vmem] * 8,
        out_specs=vmem,
        scratch_shapes=[
            pltpu.VMEM((kv, width), jnp.bfloat16),
            pltpu.VMEM((width, kv), jnp.bfloat16),
            pltpu.VMEM((tokens, width), jnp.bfloat16),
            pltpu.VMEM((tokens, 128), jnp.float32),
            pltpu.VMEM((BLOCKS, ROWS, width), jnp.bfloat16),
            pltpu.VMEM((BLOCKS, ROWS, width), jnp.bfloat16),
            pltpu.VMEM((ROWS, width), jnp.float32),
            pltpu.VMEM((tokens, kv), jnp.bfloat16),
            pltpu.VMEM((tokens, proj), jnp.float32),
            dma((2, 4, 3)), dma((2, 4, 3)), dma((10,)), dma((10,)), dma((36,)), dma((36,)),
            dma((BLOCKS,)), dma((BLOCKS,)),
        ],
        compiler_params=pltpu.CompilerParams(
            collective_id=0, has_side_effects=True, vmem_limit_bytes=48 * 1024 * 1024
        ),
        cost_estimate=pl.CostEstimate(flops=3 * 10**9, bytes_accessed=4 * 10**6, transcendentals=0),
    )(act, top, mask, gain, vt_own, ot_own, vproj, gproj)


def per_device(
    activations, top_grad, loss_mask, norm_gain, value_weight, output_weight, value_proj, grad_proj, store
):
    feat = chain(
        activations[0], top_grad, loss_mask.reshape(1, -1), norm_gain, value_weight[0].T, output_weight[0].T,
        value_proj[0], grad_proj[0],
    )
    features = feat.reshape(1, -1)
    gathered = lax.all_gather(features, "shard", axis=0, tiled=True)
    scores = lax.dot_general(
        gathered, store[0], (((1,), (1,)), ((), ())),
        precision=lax.Precision.HIGHEST, preferred_element_type=jnp.float32,
    )
    count = lax.axis_size("section")
    blocks = scores.reshape(count, scores.shape[0] // count, scores.shape[1])
    arrived = lax.all_to_all(blocks, "section", split_axis=0, concat_axis=0, tiled=True)
    return arrived.sum(axis=0)


def solution(mesh):
    placed = (
        P("section", "shard", None),
        P("shard", None),
        P("shard"),
        P("section", None),
        P("section", "shard", None),
        P("section", None, "shard"),
        P("section", None, None),
        P("section", None, None),
        P("section", "shard", None),
    )
    return jax.shard_map(
        per_device, mesh=mesh, in_specs=placed, out_specs=P("section", "shard"), check_vma=False
    )
```

```python
import jax
import jax.numpy as jnp
from jax import lax
from jax.experimental import pallas as pl
from jax.experimental.pallas import tpu as pltpu
from jax.sharding import PartitionSpec as P

LEN = 96
EPSILON = 1e-05
MESH = pl.DeviceIdType.MESH
NZ = 8
SECTIONS = 8
ROWS = 16
BLOCKS = LEN // ROWS


def chain_kernel(
    act_hbm, top_hbm, mask, gain, v_hbm, o_hbm, vproj_hbm, gproj_hbm, store_hbm,
    out,
    act, top, vproj, gproj, store, v_raw, o_raw, vt_own, ot_own, store_low,
    wvt, wot, normed, rms, c_in, c_out, scaled, va, vlow,
    feat, feat_own, feats, feat_rows, feat_all, part_out, part_in,
    ls, zs, zr, xs, xr, ds_, dr, cs, cr, fs, fr, gs, gr, ps, pr,
):
    sec = lax.axis_index("section")
    shard = lax.axis_index("shard")
    z = shard // 4
    xl = (shard // 2) % 2
    core = shard % 2
    width = act.shape[1]
    kv = wot.shape[1]
    cols = vt_own.shape[1]

    def dev(z_, x_, c_):
        return (sec, z_ * 4 + x_ * 2 + c_)

    z_next = (z + 1) % NZ
    z_prev = (z + NZ - 1) % NZ
    up = (sec + 1) % SECTIONS
    down = (sec + SECTIONS - 1) % SECTIONS
    own_v = pltpu.make_async_copy(v_hbm, v_raw, ls.at[0])
    own_o = pltpu.make_async_copy(o_hbm, o_raw, ls.at[1])
    own_v.start()
    own_o.start()
    barrier = pltpu.get_barrier_semaphore()
    peers = [dev((z + p // 2) % NZ, (xl + p) % 2, core) for p in range(1, 2 * NZ)]
    peers.append(dev(z, xl, 1 - core))
    peers.extend([((sec + d) % SECTIONS, shard) for d in range(1, SECTIONS)])
    for peer in peers:
        pl.semaphore_signal(barrier, inc=1, device_id=peer, device_id_type=MESH)
    local = [
        pltpu.make_async_copy(source, target, ls.at[2 + n])
        for n, (source, target) in enumerate(
            ((act_hbm, act), (gproj_hbm, gproj), (vproj_hbm, vproj), (store_hbm, store), (top_hbm, top))
        )
    ]
    for copy in local:
        copy.start()
    own_o.wait()
    ot_own[...] = o_raw[...].T
    own_v.wait()
    vt_own[...] = v_raw[...].T
    pl.semaphore_wait(barrier, len(peers))

    def v_block(z_, x_, c_, half):
        first = pl.multiple_of((z_ * 4 + x_ * 2 + c_) * cols, cols)
        if half is None:
            return wvt.at[:, pl.ds(first, cols)]
        return wvt.at[pl.ds(half * (kv // 2), kv // 2), pl.ds(first, cols)]

    def o_block(z_, x_, c_, half):
        first = (z_ * 4 + x_ * 2 + c_) * cols
        if half is None:
            return wot.at[pl.ds(pl.multiple_of(first, cols), cols), :]
        return wot.at[pl.ds(pl.multiple_of(first + half * (cols // 2), cols // 2), cols // 2), :]

    def block(item, z_, c_, half):
        if item == 0:
            return v_block(z_, xl, c_, half)
        return o_block(z_, xl if item == 1 else 1 - xl, c_, half)

    def origin(direction, hops):
        return (z + (NZ - hops if direction == 0 else hops)) % NZ

    def z_copy(direction, k, item):
        half = None if k < 3 else direction
        zo = origin(direction, k)
        dst = block(item, zo, core, half)
        src = (vt_own if item == 0 else ot_own) if k == 0 and item < 2 else dst
        return pltpu.make_async_remote_copy(
            src_ref=src, dst_ref=dst, send_sem=zs.at[direction, k, item], recv_sem=zr.at[direction, k, item],
            device_id=dev(z_next if direction == 0 else z_prev, xl, core), device_id_type=MESH,
        )

    def z_arrival(direction, k, item):
        half = None if k < 3 else direction
        ref = block(item, origin(direction, k + 1), core, half)
        return pltpu.make_async_remote_copy(
            src_ref=ref, dst_ref=ref, send_sem=zs.at[direction, k, item], recv_sem=zr.at[direction, k, item],
            device_id=dev(z_prev if direction == 0 else z_next, xl, core), device_id_type=MESH,
        )

    def x_refs(index, x_):
        if index == 0:
            return o_block(z, x_, core, None)
        if index == 1:
            return v_block(z, x_, core, None)
        direction, k = (index - 2) // 4, (index - 2) % 4
        return v_block(origin(direction, k + 1), x_, core, None if k < 3 else direction)

    def x_copy(index):
        dst = x_refs(index, xl)
        src = (ot_own, vt_own)[index] if index < 2 else dst
        return pltpu.make_async_remote_copy(
            src_ref=src, dst_ref=dst, send_sem=xs.at[index], recv_sem=xr.at[index],
            device_id=dev(z, 1 - xl, core), device_id_type=MESH,
        )

    def x_arrival(index):
        ref = x_refs(index, 1 - xl)
        return pltpu.make_async_remote_copy(
            src_ref=ref, dst_ref=ref, send_sem=xs.at[index], recv_sem=xr.at[index],
            device_id=dev(z, 1 - xl, core), device_id_type=MESH,
        )

    def d_refs(index, c_):
        if index == 0:
            return o_block(z, xl, c_, None)
        if index == 1:
            return v_block(z, xl, c_, None)
        if index < 26:
            direction, k, item = (index - 2) // 12, (index - 2) // 3 % 4, (index - 2) % 3
            return block(item, origin(direction, k + 1), c_, None if k < 3 else direction)
        index -= 26
        if index == 0:
            return o_block(z, 1 - xl, c_, None)
        if index == 1:
            return v_block(z, 1 - xl, c_, None)
        direction, k = (index - 2) // 4, (index - 2) % 4
        return v_block(origin(direction, k + 1), 1 - xl, c_, None if k < 3 else direction)

    def d_copy(index):
        dst = d_refs(index, core)
        src = (ot_own, vt_own)[index] if index < 2 else dst
        return pltpu.make_async_remote_copy(
            src_ref=src, dst_ref=dst, send_sem=ds_.at[index], recv_sem=dr.at[index],
            device_id=dev(z, xl, 1 - core), device_id_type=MESH,
        )

    def d_arrival(index):
        ref = d_refs(index, 1 - core)
        return pltpu.make_async_remote_copy(
            src_ref=ref, dst_ref=ref, send_sem=ds_.at[index], recv_sem=dr.at[index],
            device_id=dev(z, xl, 1 - core), device_id_type=MESH,
        )

    started = []

    def start(copy):
        copy.start()
        started.append(copy)

    start(x_copy(0))
    start(x_copy(1))
    for item in (0, 1):
        for direction in (0, 1):
            start(z_copy(direction, 0, item))
    start(d_copy(0))
    start(d_copy(1))
    own = pl.ds(pl.multiple_of(shard * cols, cols), cols)
    wvt[:, own] = vt_own[...]
    wot[own, :] = ot_own[...]

    def prepare(b, carry):
        rows = pl.ds(pl.multiple_of(b * ROWS, ROWS), ROWS)
        hidden = act[rows, :].astype(jnp.float32)
        inverse = lax.rsqrt(jnp.mean(hidden * hidden, axis=-1, keepdims=True) + EPSILON)
        rms[rows, :] = jnp.broadcast_to(inverse, (ROWS, 128))
        normed[rows, :] = (hidden * inverse * gain[...]).astype(jnp.bfloat16)
        return carry

    local[0].wait()
    lax.fori_loop(0, BLOCKS, prepare, 0)
    local[4].wait()

    @pl.when(sec == SECTIONS - 1)
    def _():
        def masked(b, carry):
            rows = pl.ds(pl.multiple_of(b * ROWS, ROWS), ROWS)
            row_at = lax.broadcasted_iota(jnp.int32, (ROWS, LEN), 0) + b * ROWS
            col_at = lax.broadcasted_iota(jnp.int32, (ROWS, LEN), 1)
            kept = jnp.where(row_at == col_at, mask[...].astype(jnp.float32), 0.0)
            column = jnp.sum(kept, axis=-1, keepdims=True)
            c_in[b] = (top[rows, :].astype(jnp.float32) * column).astype(jnp.bfloat16)
            return carry

        lax.fori_loop(0, BLOCKS, masked, 0)

    local[1].wait()
    local[2].wait()
    local[3].wait()

    def lowered(b, carry):
        rows = pl.ds(pl.multiple_of(b * ROWS, ROWS), ROWS)
        store_low[rows, :] = store[rows, :].astype(jnp.bfloat16)
        return carry

    x_arrival(0).wait_recv()
    for direction in (0, 1):
        start(z_copy(direction, 0, 2))
    start(d_copy(26))
    lax.fori_loop(0, store.shape[0] // ROWS, lowered, 0)
    x_arrival(1).wait_recv()
    start(d_copy(27))
    for k in range(4):
        for item in range(3):
            for direction in (0, 1):
                z_arrival(direction, k, item).wait_recv()
                if k < 3:
                    start(z_copy(direction, k + 1, item))
                if item == 0:
                    start(x_copy(2 + direction * 4 + k))
                start(d_copy(2 + direction * 12 + k * 3 + item))
        for direction in (0, 1):
            x_arrival(2 + direction * 4 + k).wait_recv()
            start(d_copy(26 + 2 + direction * 4 + k))
    for index in range(36):
        d_arrival(index).wait_recv()

    def value_path():
        for n in range(0, kv, 256):
            part = lax.dot_general(
                normed[...], wvt[n : n + 256, :], (((1,), (1,)), ((), ())), preferred_element_type=jnp.float32
            )
            va[:, n : n + 256] = part.astype(jnp.bfloat16)
        vlow[...] = lax.dot_general(
            va[...], vproj[...], (((1,), (1,)), ((), ())), preferred_element_type=jnp.float32
        )

    def c_copy(b):
        return pltpu.make_async_remote_copy(
            src_ref=c_out.at[b], dst_ref=c_in.at[b], send_sem=cs.at[b], recv_sem=cr.at[b],
            device_id=(down, shard), device_id_type=MESH,
        )

    def c_arrival(b):
        return pltpu.make_async_remote_copy(
            src_ref=c_in.at[b], dst_ref=c_in.at[b], send_sem=cs.at[b], recv_sem=cr.at[b],
            device_id=(up, shard), device_id_type=MESH,
        )

    @pl.when(sec < SECTIONS - 1)
    def _():
        value_path()

    def stage(b, carry):
        @pl.when(sec < SECTIONS - 1)
        def _():
            c_arrival(b).wait_recv()

        @pl.when(sec > 0)
        def _():
            rows = pl.ds(pl.multiple_of(b * ROWS, ROWS), ROWS)
            grad_value = jnp.dot(c_in[b], wot[...], preferred_element_type=jnp.float32).astype(jnp.bfloat16)
            total = jnp.zeros((ROWS, 1), jnp.float32)
            step = 512
            for n in range(0, width, step):
                part = jnp.dot(grad_value, wvt[:, n : n + step], preferred_element_type=jnp.float32)
                part = gain[:, n : n + step] * part
                scaled[:, n : n + step] = part
                hidden = act[rows, n : n + step].astype(jnp.float32)
                total += jnp.sum(part * hidden, axis=-1, keepdims=True)
            inverse = rms[rows, :][:, :1]
            back = (inverse * inverse * inverse) * (total / width)
            for n in range(0, width, step):
                hidden = act[rows, n : n + step].astype(jnp.float32)
                grad_input = inverse * scaled[:, n : n + step] - hidden * back
                c_out[b, :, n : n + step] = (
                    c_in[b, :, n : n + step].astype(jnp.float32) + grad_input
                ).astype(jnp.bfloat16)
            c_copy(b).start()

        return carry

    lax.fori_loop(0, BLOCKS, stage, 0)

    @pl.when(sec == SECTIONS - 1)
    def _():
        value_path()

    low = lax.dot_general(
        c_in[...].reshape(LEN, width), gproj[...], (((1,), (1,)), ((), ())), preferred_element_type=jnp.float32
    )
    proj = low.shape[1]
    half_rows = proj // 2
    feat[...] = lax.dot_general(
        low, vlow[...], (((0,), (0,)), ((), ())),
        precision=lax.Precision.HIGHEST, preferred_element_type=jnp.float32,
    )
    even = feat[pl.ds(0, half_rows, stride=2), :]
    odd = feat[pl.ds(1, half_rows, stride=2), :]
    packed = jnp.concatenate([even, odd], axis=1).astype(jnp.bfloat16)
    feat_own[...] = packed
    feats[shard] = packed

    def slot(p, c_):
        return ((z + NZ - p // 2) % NZ) * 4 + ((xl + p) % 2) * 2 + c_

    def f_copy(p):
        return pltpu.make_async_remote_copy(
            src_ref=feat_own, dst_ref=feats.at[shard], send_sem=fs.at[p], recv_sem=fr.at[p],
            device_id=dev((z + p // 2) % NZ, (xl + p) % 2, core), device_id_type=MESH,
        )

    def f_arrival(p):
        ref = feats.at[slot(p, core)]
        return pltpu.make_async_remote_copy(
            src_ref=ref, dst_ref=ref, send_sem=fs.at[p], recv_sem=fr.at[p],
            device_id=dev((z + NZ - p // 2) % NZ, (xl + p) % 2, core), device_id_type=MESH,
        )

    def g_copy(p):
        ref = feats.at[slot(p, core)]
        return pltpu.make_async_remote_copy(
            src_ref=feat_own if p == 0 else ref, dst_ref=ref, send_sem=gs.at[p], recv_sem=gr.at[p],
            device_id=dev(z, xl, 1 - core), device_id_type=MESH,
        )

    def g_arrival(p):
        ref = feats.at[slot(p, 1 - core)]
        return pltpu.make_async_remote_copy(
            src_ref=ref, dst_ref=ref, send_sem=gs.at[p], recv_sem=gr.at[p],
            device_id=dev(z, xl, 1 - core), device_id_type=MESH,
        )

    near = (0, 1, 7, 2, 6, 3, 5, 4)
    order = [2 * dz + dx for dz in near for dx in (0, 1)][1:]
    for p in reversed(order):
        start(f_copy(p))
    start(g_copy(0))
    for p in order:
        f_arrival(p).wait_recv()
        start(g_copy(p))
    for p in [0] + order:
        g_arrival(p).wait_recv()
    gens = feats.shape[0]
    for q in range(gens):
        feat_rows[q * half_rows : (q + 1) * half_rows, :] = feats[q].astype(jnp.float32)
    for i in range(half_rows):
        feat_all[:, i * 128 : (i + 1) * 128] = feat_rows[pl.ds(i, gens, stride=half_rows), :].astype(jnp.bfloat16)
    scores = lax.dot_general(
        feat_all[...], store_low[...], (((1,), (1,)), ((), ())), preferred_element_type=jnp.float32
    )
    gens_each = gens // SECTIONS
    for n in range(SECTIONS):
        part_out[n] = scores[n * gens_each : (n + 1) * gens_each, :]

    def p_copy(d):
        return pltpu.make_async_remote_copy(
            src_ref=part_out.at[(sec + d) % SECTIONS], dst_ref=part_in.at[d], send_sem=ps.at[d], recv_sem=pr.at[d],
            device_id=((sec + d) % SECTIONS, shard), device_id_type=MESH,
        )

    def p_arrival(d):
        return pltpu.make_async_remote_copy(
            src_ref=part_in.at[d], dst_ref=part_in.at[d], send_sem=ps.at[d], recv_sem=pr.at[d],
            device_id=((sec + SECTIONS - d) % SECTIONS, shard), device_id_type=MESH,
        )

    for d in range(1, SECTIONS):
        start(p_copy(d))
    total_scores = part_out[sec]
    for d in range(1, SECTIONS):
        p_arrival(d).wait_recv()
        total_scores += part_in[d]
    out[...] = total_scores
    for copy in started:
        copy.wait_send()

    @pl.when(sec > 0)
    def _():
        def sent(b, carry):
            c_copy(b).wait_send()
            return carry

        lax.fori_loop(0, BLOCKS, sent, 0)


def chain(act, top, mask, gain, v_own, o_own, vproj, gproj, store):
    tokens, width = act.shape
    kv = v_own.shape[1]
    proj = vproj.shape[0]
    examples = store.shape[0]
    gens = NZ * 4
    vmem = pl.BlockSpec(memory_space=pltpu.VMEM)
    hbm = pl.BlockSpec(memory_space=pltpu.HBM)
    dma = pltpu.SemaphoreType.DMA
    bf16, f32 = jnp.bfloat16, jnp.float32
    return pl.pallas_call(
        chain_kernel,
        out_shape=jax.ShapeDtypeStruct((gens // SECTIONS, examples), f32),
        in_specs=[hbm, hbm, vmem, vmem] + [hbm] * 5,
        out_specs=vmem,
        scratch_shapes=[
            pltpu.VMEM(act.shape, bf16),
            pltpu.VMEM(top.shape, bf16),
            pltpu.VMEM(vproj.shape, bf16),
            pltpu.VMEM(gproj.shape, bf16),
            pltpu.VMEM(store.shape, f32),
            pltpu.VMEM(v_own.shape, bf16),
            pltpu.VMEM(o_own.shape, bf16),
            pltpu.VMEM(v_own.shape[::-1], bf16),
            pltpu.VMEM(o_own.shape[::-1], bf16),
            pltpu.VMEM(store.shape, bf16),
            pltpu.VMEM((kv, width), bf16),
            pltpu.VMEM((width, kv), bf16),
            pltpu.VMEM((tokens, width), bf16),
            pltpu.VMEM((tokens, 128), f32),
            pltpu.VMEM((BLOCKS, ROWS, width), bf16),
            pltpu.VMEM((BLOCKS, ROWS, width), bf16),
            pltpu.VMEM((ROWS, width), f32),
            pltpu.VMEM((tokens, kv), bf16),
            pltpu.VMEM((tokens, proj), f32),
            pltpu.VMEM((proj, proj), f32),
            pltpu.VMEM((proj // 2, 2 * proj), bf16),
            pltpu.VMEM((gens, proj // 2, 2 * proj), bf16),
            pltpu.VMEM((gens * proj // 2, 2 * proj), f32),
            pltpu.VMEM((gens, proj * proj), bf16),
            pltpu.VMEM((SECTIONS, gens // SECTIONS, examples), f32),
            pltpu.VMEM((SECTIONS, gens // SECTIONS, examples), f32),
            dma((7,)),
            dma((2, 4, 3)), dma((2, 4, 3)), dma((10,)), dma((10,)), dma((36,)), dma((36,)),
            dma((BLOCKS,)), dma((BLOCKS,)),
            dma((2 * NZ,)), dma((2 * NZ,)), dma((2 * NZ,)), dma((2 * NZ,)), dma((SECTIONS,)), dma((SECTIONS,)),
        ],
        compiler_params=pltpu.CompilerParams(
            collective_id=0, has_side_effects=True, vmem_limit_bytes=60 * 1024 * 1024
        ),
        cost_estimate=pl.CostEstimate(flops=3 * 10**9, bytes_accessed=4 * 10**6, transcendentals=0),
    )(act, top, mask, gain, v_own, o_own, vproj, gproj, store)


def per_device(
    activations, top_grad, loss_mask, norm_gain, value_weight, output_weight, value_proj, grad_proj, store
):
    return chain(
        activations[0], top_grad, loss_mask.reshape(1, -1), norm_gain, value_weight[0], output_weight[0],
        value_proj[0].T, grad_proj[0].T, store[0],
    )


def solution(mesh):
    placed = (
        P("section", "shard", None),
        P("shard", None),
        P("shard"),
        P("section", None),
        P("section", "shard", None),
        P("section", None, "shard"),
        P("section", None, None),
        P("section", None, None),
        P("section", "shard", None),
    )
    return jax.shard_map(
        per_device, mesh=mesh, in_specs=placed, out_specs=P("section", "shard"), check_vma=False
    )
```

```python
import jax
import jax.numpy as jnp
from jax import lax
from jax.experimental import pallas as pl
from jax.experimental.pallas import tpu as pltpu
from jax.sharding import PartitionSpec as P

LEN = 96
EPSILON = 1e-05
MESH = pl.DeviceIdType.MESH
NZ = 8
SECTIONS = 8
ROWS = 16
BLOCKS = LEN // ROWS
PIECES = 4


def chain_kernel(
    act_hbm, top_hbm, mask, gain, v_hbm, o_hbm, vproj_hbm, gproj_hbm, store_hbm,
    out,
    act, top, vproj, gproj, store, v_raw, o_raw, vt_own, ot_own, store_low,
    wvt, wot, held, normed, rms, c_in, c_out, va_sum, va, vlow,
    feat, feat_own, feats, feat_rows, feat_all, part_out, part_in,
    ls, zs, zr, xs, xr, ds_, dr, hs, hr, cs, cr, fs, fr, gs, gr, ps, pr,
):
    sec = lax.axis_index("section")
    shard = lax.axis_index("shard")
    z = shard // 4
    xl = (shard // 2) % 2
    core = shard % 2
    width = act.shape[1]
    kv = wot.shape[1]
    cols = vt_own.shape[1]

    def dev(z_, x_, c_):
        return (sec, z_ * 4 + x_ * 2 + c_)

    z_next = (z + 1) % NZ
    z_prev = (z + NZ - 1) % NZ
    up = (sec + 1) % SECTIONS
    down = (sec + SECTIONS - 1) % SECTIONS
    own_v = pltpu.make_async_copy(v_hbm, v_raw, ls.at[0])
    own_o = pltpu.make_async_copy(o_hbm, o_raw, ls.at[1])
    own_v.start()
    own_o.start()
    barrier = pltpu.get_barrier_semaphore()
    peers = [dev((z + p // 2) % NZ, (xl + p) % 2, core) for p in range(1, 2 * NZ)]
    outer = ((sec + SECTIONS // 2) % SECTIONS, z * 4 + (1 - xl) * 2 + core)
    peers.append(outer)
    peers.append(dev(z, xl, 1 - core))
    peers.extend([((sec + d) % SECTIONS, shard) for d in range(1, SECTIONS)])
    for peer in peers:
        pl.semaphore_signal(barrier, inc=1, device_id=peer, device_id_type=MESH)
    local = [
        pltpu.make_async_copy(source, target, ls.at[2 + n])
        for n, (source, target) in enumerate(
            ((act_hbm, act), (gproj_hbm, gproj), (vproj_hbm, vproj), (store_hbm, store), (top_hbm, top))
        )
    ]
    for copy in local:
        copy.start()
    own_o.wait()
    ot_own[...] = o_raw[...].T
    own_v.wait()
    vt_own[...] = v_raw[...].T
    pl.semaphore_wait(barrier, len(peers))

    def v_block(z_, x_, c_, half):
        first = pl.multiple_of((z_ * 4 + x_ * 2 + c_) * cols, cols)
        if half is None:
            return wvt.at[:, pl.ds(first, cols)]
        return wvt.at[pl.ds(half * (kv // 2), kv // 2), pl.ds(first, cols)]

    def o_block(z_, x_, c_, span):
        begin, size = span
        first = pl.multiple_of((z_ * 4 + x_ * 2 + c_) * cols + begin, 16)
        return wot.at[pl.ds(first, size), :]

    def o_span(item, k, direction, client):
        begin, size = 0, cols
        if item == 3 or (item == 1 and client):
            size = cols // 2
            begin = 0 if item == 3 else cols // 2
        if k == 3:
            size = size // 2
            begin += direction * size
        return begin, size

    def block(item, z_, c_, k, direction, client):
        if item == 0:
            return v_block(z_, xl, c_, None if k < 3 else direction)
        span = o_span(item, k, direction, client)
        if item == 3:
            return held.at[z_, pl.ds(*span), :]
        return o_block(z_, xl if item == 1 else 1 - xl, c_, span)

    def origin(direction, hops):
        return (z + (NZ - hops if direction == 0 else hops)) % NZ

    def remote(src, dst, sends, recvs, index, peer):
        return pltpu.make_async_remote_copy(
            src_ref=src, dst_ref=dst, send_sem=sends.at[index], recv_sem=recvs.at[index],
            device_id=peer, device_id_type=MESH,
        )

    def z_copy(direction, k, item, client):
        dst = block(item, origin(direction, k), core, k, direction, client)
        src = dst
        if k == 0 and item == 0:
            src = vt_own
        if k == 0 and item == 1:
            src = ot_own.at[pl.ds(*o_span(1, 0, direction, client)), :]
        return remote(src, dst, zs, zr, (direction, k, item), dev(z_next if direction == 0 else z_prev, xl, core))

    def z_arrival(direction, k, item, client):
        ref = block(item, origin(direction, k + 1), core, k, direction, client)
        return remote(ref, ref, zs, zr, (direction, k, item), dev(z_prev if direction == 0 else z_next, xl, core))

    def x_refs(index, x_):
        if index == 0:
            return o_block(z, x_, core, (0, cols))
        if index == 1:
            return v_block(z, x_, core, None)
        direction, k = (index - 2) // 4, (index - 2) % 4
        return v_block(origin(direction, k + 1), x_, core, None if k < 3 else direction)

    def x_copy(index):
        dst = x_refs(index, xl)
        return remote((ot_own, vt_own)[index] if index < 2 else dst, dst, xs, xr, index, dev(z, 1 - xl, core))

    def x_arrival(index):
        ref = x_refs(index, 1 - xl)
        return remote(ref, ref, xs, xr, index, dev(z, 1 - xl, core))

    def d_refs(index, c_, client):
        if index == 0:
            return o_block(z, xl, c_, (0, cols))
        if index == 1:
            return v_block(z, xl, c_, None)
        if index < 26:
            direction, k, item = (index - 2) // 12, (index - 2) // 3 % 4, (index - 2) % 3
            return block(item, origin(direction, k + 1), c_, k, direction, client)
        if index == 26:
            return o_block(z, 1 - xl, c_, (0, cols))
        if index == 27:
            return v_block(z, 1 - xl, c_, None)
        if index < 36:
            direction, k = (index - 28) // 4, (index - 28) % 4
            return v_block(origin(direction, k + 1), 1 - xl, c_, None if k < 3 else direction)
        direction, k = (index - 36) // 4, (index - 36) % 4
        return o_block(origin(direction, k + 1), xl, c_, o_span(3, k, direction, client))

    def d_copy(index, client):
        dst = d_refs(index, core, client)
        return remote((ot_own, vt_own)[index] if index < 2 else dst, dst, ds_, dr, index, dev(z, xl, 1 - core))

    def d_arrival(index, client):
        ref = d_refs(index, 1 - core, client)
        return remote(ref, ref, ds_, dr, index, dev(z, xl, 1 - core))

    def lent_copy():
        return remote(ot_own.at[pl.ds(0, cols // 2), :], held.at[z], hs, hr, 0, outer)

    def lent_arrival():
        return remote(held.at[z], held.at[z], hs, hr, 0, outer)

    def back_copy(direction, k):
        zo = origin(direction, k + 1)
        span = o_span(3, k, direction, True)
        return remote(
            held.at[zo, pl.ds(*span), :], o_block(zo, 1 - xl, core, span), hs, hr, 1 + direction * 4 + k, outer
        )

    def back_arrival(direction, k):
        ref = o_block(origin(direction, k + 1), xl, core, o_span(3, k, direction, True))
        return remote(ref, ref, hs, hr, 1 + direction * 4 + k, outer)

    started = {True: [], False: [], None: []}

    def start(role, make, *given):
        make(*given).start()
        started[role].append((make, given))

    def value_pair(z_, x_):
        span = pl.ds(pl.multiple_of((z_ * 4 + x_ * 2) * cols, 2 * cols), 2 * cols)
        left = normed[:, span]
        for n in range(0, kv, 256):
            va_sum[:, n : n + 256] += lax.dot_general(
                left, wvt[n : n + 256, span], (((1,), (1,)), ((), ())), preferred_element_type=jnp.float32
            )

    def pairs_of(k, client):
        if k < 0:
            for index in (1, 27):
                d_arrival(index, client).wait_recv()
            value_pair(z, 0)
            value_pair(z, 1)
            return
        for direction in (0, 1):
            d_arrival(2 + direction * 12 + k * 3, client).wait_recv()
            d_arrival(28 + direction * 4 + k, client).wait_recv()
            if k < 3 or direction == 1:
                value_pair(origin(direction, k + 1), 0)
                value_pair(origin(direction, k + 1), 1)

    def begin(client):
        start(client, x_copy, 0)
        start(client, x_copy, 1)
        if client:
            start(client, lent_copy)
        for item in (0, 1) if client else (0,):
            for direction in (0, 1):
                start(client, z_copy, direction, 0, item, client)
        start(client, d_copy, 0, client)
        start(client, d_copy, 1, client)

    def z_step(direction, k, item, client):
        z_arrival(direction, k, item, client).wait_recv()
        if k < 3:
            start(client, z_copy, direction, k + 1, item, client)
        if item == 0:
            start(client, x_copy, 2 + direction * 4 + k)
        if item == 3:
            start(client, back_copy, direction, k)
        else:
            start(client, d_copy, 2 + direction * 12 + k * 3 + item, client)

    def x_step(k, client):
        for direction in (0, 1):
            x_arrival(2 + direction * 4 + k).wait_recv()
            start(client, d_copy, 28 + direction * 4 + k, client)

    def last_waits(client):
        pairs_of(3, client)
        late = [0, 26] + [2 + direction * 12 + k * 3 + item for direction in (0, 1) for k in range(4) for item in (1, 2)]
        if client:
            late += range(36, 44)
        for index in late:
            d_arrival(index, client).wait_recv()

    def gather_client():
        x_arrival(0).wait_recv()
        for direction in (0, 1):
            start(True, z_copy, direction, 0, 2, True)
        start(True, d_copy, 26, True)
        x_arrival(1).wait_recv()
        start(True, d_copy, 27, True)
        for k in range(4):
            for item in (0, 1):
                for direction in (0, 1):
                    z_step(direction, k, item, True)
            if k == 3:
                x_step(k, True)
                pairs_of(k - 1, True)
            for direction in (0, 1):
                back_arrival(direction, k).wait_recv()
                start(True, d_copy, 36 + direction * 4 + k, True)
            for direction in (0, 1):
                z_step(direction, k, 2, True)
            if k < 3:
                x_step(k, True)
                pairs_of(k - 1, True)
        last_waits(True)

    def gather_helper():
        lent_arrival().wait_recv()
        for direction in (0, 1):
            start(False, z_copy, direction, 0, 3, False)
        x_arrival(0).wait_recv()
        start(False, d_copy, 26, False)
        for k in range(4):
            if k == 3:
                for item in (1, 2):
                    for direction in (0, 1):
                        start(False, z_copy, direction, 0, item, False)
            for item in (0, 3):
                for direction in (0, 1):
                    z_step(direction, k, item, False)
        x_arrival(1).wait_recv()
        start(False, d_copy, 27, False)
        for k in range(4):
            for item in (1, 2):
                for direction in (0, 1):
                    z_step(direction, k, item, False)
            x_step(k, False)
            pairs_of(k - 1, False)
        last_waits(False)

    half_of = SECTIONS // 2

    @pl.when(sec >= half_of)
    def _():
        begin(True)

    @pl.when(sec < half_of)
    def _():
        begin(False)

    own = pl.ds(pl.multiple_of(shard * cols, cols), cols)
    wvt[:, own] = vt_own[...]
    wot[own, :] = ot_own[...]

    def prepare(b, carry):
        rows = pl.ds(pl.multiple_of(b * ROWS, ROWS), ROWS)
        hidden = act[rows, :].astype(jnp.float32)
        inverse = lax.rsqrt(jnp.mean(hidden * hidden, axis=-1, keepdims=True) + EPSILON)
        rms[rows, :] = jnp.broadcast_to(inverse, (ROWS, 128))
        normed[rows, :] = (hidden * inverse * gain[...]).astype(jnp.bfloat16)
        return carry

    local[0].wait()
    lax.fori_loop(0, BLOCKS, prepare, 0)
    local[4].wait()

    @pl.when(sec == SECTIONS - 1)
    def _():
        def masked(b, carry):
            rows = pl.ds(pl.multiple_of(b * ROWS, ROWS), ROWS)
            row_at = lax.broadcasted_iota(jnp.int32, (ROWS, LEN), 0) + b * ROWS
            col_at = lax.broadcasted_iota(jnp.int32, (ROWS, LEN), 1)
            kept = jnp.where(row_at == col_at, mask[...].astype(jnp.float32), 0.0)
            column = jnp.sum(kept, axis=-1, keepdims=True)
            c_in[b] = (top[rows, :].astype(jnp.float32) * column).astype(jnp.bfloat16)
            return carry

        lax.fori_loop(0, BLOCKS, masked, 0)

    local[1].wait()
    local[2].wait()
    local[3].wait()

    def lowered(b, carry):
        rows = pl.ds(pl.multiple_of(b * ROWS, ROWS), ROWS)
        store_low[rows, :] = store[rows, :].astype(jnp.bfloat16)
        return carry

    lax.fori_loop(0, store.shape[0] // ROWS, lowered, 0)
    va_sum[...] = jnp.zeros_like(va_sum)

    @pl.when(sec >= half_of)
    def _():
        gather_client()

    @pl.when(sec < half_of)
    def _():
        gather_helper()

    def value_path():
        va[...] = va_sum[...].astype(jnp.bfloat16)
        vlow[...] = lax.dot_general(
            va[...], vproj[...], (((1,), (1,)), ((), ())), preferred_element_type=jnp.float32
        )

    piece = width // PIECES

    def c_copy(b, n):
        span = pl.ds(n * piece, piece)
        return pltpu.make_async_remote_copy(
            src_ref=c_out.at[b, :, span], dst_ref=c_in.at[b, :, span], send_sem=cs.at[b, n], recv_sem=cr.at[b, n],
            device_id=(down, shard), device_id_type=MESH,
        )

    def c_arrival(b, n):
        ref = c_in.at[b, :, pl.ds(n * piece, piece)]
        return pltpu.make_async_remote_copy(
            src_ref=ref, dst_ref=ref, send_sem=cs.at[b, n], recv_sem=cr.at[b, n],
            device_id=(up, shard), device_id_type=MESH,
        )

    def arrived(b, pieces):
        @pl.when(sec < SECTIONS - 1)
        def _():
            for n in pieces:
                c_arrival(b, n).wait_recv()

    @pl.when(sec < SECTIONS - 1)
    def _():
        value_path()

    def stage(b, carry):
        @pl.when(sec == 0)
        def _():
            arrived(b, range(PIECES))

        @pl.when(sec > 0)
        def _():
            rows = pl.ds(pl.multiple_of(b * ROWS, ROWS), ROWS)
            split = width - piece
            arrived(b, range(PIECES - 1))
            grad_value = jnp.dot(c_in[b, :, :split], wot[:split, :], preferred_element_type=jnp.float32)
            arrived(b, (PIECES - 1,))
            grad_value += jnp.dot(c_in[b, :, split:], wot[split:, :], preferred_element_type=jnp.float32)
            grad_value = grad_value.astype(jnp.bfloat16)
            inverse = rms[rows, :][:, :1]
            total = jnp.sum(grad_value.astype(jnp.float32) * va_sum[rows, :], axis=-1, keepdims=True)
            back = (inverse * inverse) * (total / width)
            for n in range(PIECES):
                span = slice(n * piece, (n + 1) * piece)
                part = gain[:, span] * jnp.dot(grad_value, wvt[:, span], preferred_element_type=jnp.float32)
                hidden = act[rows, span].astype(jnp.float32)
                grad_input = inverse * part - hidden * back
                c_out[b, :, span] = (c_in[b, :, span].astype(jnp.float32) + grad_input).astype(jnp.bfloat16)
                c_copy(b, n).start()

        return carry

    lax.fori_loop(0, BLOCKS, stage, 0)

    @pl.when(sec == SECTIONS - 1)
    def _():
        value_path()

    low = lax.dot_general(
        c_in[...].reshape(LEN, width), gproj[...], (((1,), (1,)), ((), ())), preferred_element_type=jnp.float32
    )
    proj = low.shape[1]
    half_rows = proj // 2
    feat[...] = lax.dot_general(
        low, vlow[...], (((0,), (0,)), ((), ())),
        precision=lax.Precision.HIGHEST, preferred_element_type=jnp.float32,
    )
    even = feat[pl.ds(0, half_rows, stride=2), :]
    odd = feat[pl.ds(1, half_rows, stride=2), :]
    packed = jnp.concatenate([even, odd], axis=1).astype(jnp.bfloat16)
    feat_own[...] = packed
    feats[shard] = packed

    def slot(p, c_):
        return ((z + NZ - p // 2) % NZ) * 4 + ((xl + p) % 2) * 2 + c_

    def f_copy(p):
        return pltpu.make_async_remote_copy(
            src_ref=feat_own, dst_ref=feats.at[shard], send_sem=fs.at[p], recv_sem=fr.at[p],
            device_id=dev((z + p // 2) % NZ, (xl + p) % 2, core), device_id_type=MESH,
        )

    def f_arrival(p):
        ref = feats.at[slot(p, core)]
        return pltpu.make_async_remote_copy(
            src_ref=ref, dst_ref=ref, send_sem=fs.at[p], recv_sem=fr.at[p],
            device_id=dev((z + NZ - p // 2) % NZ, (xl + p) % 2, core), device_id_type=MESH,
        )

    def g_copy(p):
        ref = feats.at[slot(p, core)]
        return pltpu.make_async_remote_copy(
            src_ref=feat_own if p == 0 else ref, dst_ref=ref, send_sem=gs.at[p], recv_sem=gr.at[p],
            device_id=dev(z, xl, 1 - core), device_id_type=MESH,
        )

    def g_arrival(p):
        ref = feats.at[slot(p, 1 - core)]
        return pltpu.make_async_remote_copy(
            src_ref=ref, dst_ref=ref, send_sem=gs.at[p], recv_sem=gr.at[p],
            device_id=dev(z, xl, 1 - core), device_id_type=MESH,
        )

    near = (0, 1, 7, 2, 6, 3, 5, 4)
    order = [2 * dz + dx for dz in near for dx in (0, 1)][1:]
    for p in reversed(order):
        start(None, f_copy, p)
    start(None, g_copy, 0)
    for p in order:
        f_arrival(p).wait_recv()
        start(None, g_copy, p)
    for p in [0] + order:
        g_arrival(p).wait_recv()
    gens = feats.shape[0]
    for q in range(gens):
        feat_rows[q * half_rows : (q + 1) * half_rows, :] = feats[q].astype(jnp.float32)
    for i in range(half_rows):
        feat_all[:, i * 128 : (i + 1) * 128] = feat_rows[pl.ds(i, gens, stride=half_rows), :].astype(jnp.bfloat16)
    scores = lax.dot_general(
        feat_all[...], store_low[...], (((1,), (1,)), ((), ())), preferred_element_type=jnp.float32
    )
    gens_each = gens // SECTIONS
    for n in range(SECTIONS):
        part_out[n] = scores[n * gens_each : (n + 1) * gens_each, :]

    def p_copy(d):
        return pltpu.make_async_remote_copy(
            src_ref=part_out.at[(sec + d) % SECTIONS], dst_ref=part_in.at[d], send_sem=ps.at[d], recv_sem=pr.at[d],
            device_id=((sec + d) % SECTIONS, shard), device_id_type=MESH,
        )

    def p_arrival(d):
        return pltpu.make_async_remote_copy(
            src_ref=part_in.at[d], dst_ref=part_in.at[d], send_sem=ps.at[d], recv_sem=pr.at[d],
            device_id=((sec + SECTIONS - d) % SECTIONS, shard), device_id_type=MESH,
        )

    for d in range(1, SECTIONS):
        start(None, p_copy, d)
    total_scores = part_out[sec]
    for d in range(1, SECTIONS):
        p_arrival(d).wait_recv()
        total_scores += part_in[d]
    out[...] = total_scores
    for make, given in started[None]:
        make(*given).wait_send()

    @pl.when(sec >= half_of)
    def _():
        for make, given in started[True]:
            make(*given).wait_send()

    @pl.when(sec < half_of)
    def _():
        for make, given in started[False]:
            make(*given).wait_send()

    @pl.when(sec > 0)
    def _():
        def sent(b, carry):
            for n in range(PIECES):
                c_copy(b, n).wait_send()
            return carry

        lax.fori_loop(0, BLOCKS, sent, 0)


def chain(act, top, mask, gain, v_own, o_own, vproj, gproj, store):
    tokens, width = act.shape
    kv = v_own.shape[1]
    proj = vproj.shape[0]
    examples = store.shape[0]
    gens = NZ * 4
    vmem = pl.BlockSpec(memory_space=pltpu.VMEM)
    hbm = pl.BlockSpec(memory_space=pltpu.HBM)
    dma = pltpu.SemaphoreType.DMA
    bf16, f32 = jnp.bfloat16, jnp.float32
    return pl.pallas_call(
        chain_kernel,
        out_shape=jax.ShapeDtypeStruct((gens // SECTIONS, examples), f32),
        in_specs=[hbm, hbm, vmem, vmem] + [hbm] * 5,
        out_specs=vmem,
        scratch_shapes=[
            pltpu.VMEM(act.shape, bf16),
            pltpu.VMEM(top.shape, bf16),
            pltpu.VMEM(vproj.shape, bf16),
            pltpu.VMEM(gproj.shape, bf16),
            pltpu.VMEM(store.shape, f32),
            pltpu.VMEM(v_own.shape, bf16),
            pltpu.VMEM(o_own.shape, bf16),
            pltpu.VMEM(v_own.shape[::-1], bf16),
            pltpu.VMEM(o_own.shape[::-1], bf16),
            pltpu.VMEM(store.shape, bf16),
            pltpu.VMEM((kv, width), bf16),
            pltpu.VMEM((width, kv), bf16),
            pltpu.VMEM((NZ, v_own.shape[0] // 2, kv), bf16),
            pltpu.VMEM((tokens, width), bf16),
            pltpu.VMEM((tokens, 128), f32),
            pltpu.VMEM((BLOCKS, ROWS, width), bf16),
            pltpu.VMEM((BLOCKS, ROWS, width), bf16),
            pltpu.VMEM((tokens, kv), f32),
            pltpu.VMEM((tokens, kv), bf16),
            pltpu.VMEM((tokens, proj), f32),
            pltpu.VMEM((proj, proj), f32),
            pltpu.VMEM((proj // 2, 2 * proj), bf16),
            pltpu.VMEM((gens, proj // 2, 2 * proj), bf16),
            pltpu.VMEM((gens * proj // 2, 2 * proj), f32),
            pltpu.VMEM((gens, proj * proj), bf16),
            pltpu.VMEM((SECTIONS, gens // SECTIONS, examples), f32),
            pltpu.VMEM((SECTIONS, gens // SECTIONS, examples), f32),
            dma((7,)),
            dma((2, 4, 4)), dma((2, 4, 4)), dma((10,)), dma((10,)), dma((44,)), dma((44,)), dma((9,)), dma((9,)),
            dma((BLOCKS, PIECES)), dma((BLOCKS, PIECES)),
            dma((2 * NZ,)), dma((2 * NZ,)), dma((2 * NZ,)), dma((2 * NZ,)), dma((SECTIONS,)), dma((SECTIONS,)),
        ],
        compiler_params=pltpu.CompilerParams(
            collective_id=0, has_side_effects=True, vmem_limit_bytes=60 * 1024 * 1024
        ),
        cost_estimate=pl.CostEstimate(flops=3 * 10**9, bytes_accessed=4 * 10**6, transcendentals=0),
    )(act, top, mask, gain, v_own, o_own, vproj, gproj, store)


def per_device(
    activations, top_grad, loss_mask, norm_gain, value_weight, output_weight, value_proj, grad_proj, store
):
    return chain(
        activations[0], top_grad, loss_mask.reshape(1, -1), norm_gain, value_weight[0], output_weight[0],
        value_proj[0].T, grad_proj[0].T, store[0],
    )


def solution(mesh):
    placed = (
        P("section", "shard", None),
        P("shard", None),
        P("shard"),
        P("section", None),
        P("section", "shard", None),
        P("section", None, "shard"),
        P("section", None, None),
        P("section", None, None),
        P("section", "shard", None),
    )
    return jax.shard_map(
        per_device, mesh=mesh, in_specs=placed, out_specs=P("section", "shard"), check_vma=False
    )
```

```python
import jax
import jax.numpy as jnp
from jax import lax
from jax.experimental import pallas as pl
from jax.experimental.pallas import tpu as pltpu
from jax.sharding import PartitionSpec as P

LEN = 96
EPSILON = 1e-05
MESH = pl.DeviceIdType.MESH
NZ = 8
SECTIONS = 8
ROWS = 16
BLOCKS = LEN // ROWS
PIECES = 4
GROUPS = ((0, 3), (3, 4))


def chain_kernel(
    act_hbm, top_hbm, mask, gain, v_hbm, o_hbm, vproj_hbm, gproj_hbm, store_hbm,
    out,
    act, top, vproj, gproj, store, v_raw, o_raw, vt_own, ot_own, store_low,
    wvt, wot, held, normed, rms, c_in, c_out, va_sum, va, vlow,
    feat, feat_own, feats, feat_rows, feat_all, part_out, part_in,
    ls, zs, zr, xs, xr, ds_, dr, hs, hr, cs, cr, fs, fr, gs, gr, ps, pr,
):
    sec = lax.axis_index("section")
    shard = lax.axis_index("shard")
    z = shard // 4
    xl = (shard // 2) % 2
    core = shard % 2
    width = act.shape[1]
    kv = wot.shape[1]
    cols = vt_own.shape[1]

    def dev(z_, x_, c_):
        return (sec, z_ * 4 + x_ * 2 + c_)

    z_next = (z + 1) % NZ
    z_prev = (z + NZ - 1) % NZ
    up = (sec + 1) % SECTIONS
    down = (sec + SECTIONS - 1) % SECTIONS
    own_v = pltpu.make_async_copy(v_hbm, v_raw, ls.at[0])
    own_o = pltpu.make_async_copy(o_hbm, o_raw, ls.at[1])
    own_v.start()
    own_o.start()
    barrier = pltpu.get_barrier_semaphore()
    peers = [dev((z + p // 2) % NZ, (xl + p) % 2, core) for p in range(1, 2 * NZ)]
    outer = ((sec + SECTIONS // 2) % SECTIONS, z * 4 + (1 - xl) * 2 + core)
    peers.append(outer)
    peers.append(dev(z, xl, 1 - core))
    peers.extend([((sec + d) % SECTIONS, shard) for d in range(1, SECTIONS)])
    for peer in peers:
        pl.semaphore_signal(barrier, inc=1, device_id=peer, device_id_type=MESH)
    local = [
        pltpu.make_async_copy(source, target, ls.at[2 + n])
        for n, (source, target) in enumerate(
            ((act_hbm, act), (gproj_hbm, gproj), (vproj_hbm, vproj), (store_hbm, store), (top_hbm, top))
        )
    ]
    for copy in local:
        copy.start()
    own_o.wait()
    ot_own[...] = o_raw[...].T
    own_v.wait()
    vt_own[...] = v_raw[...].T
    pl.semaphore_wait(barrier, len(peers))

    def v_block(z_, x_, c_, half):
        first = pl.multiple_of((z_ * 4 + x_ * 2 + c_) * cols, cols)
        if half is None:
            return wvt.at[:, pl.ds(first, cols)]
        return wvt.at[pl.ds(half * (kv // 2), kv // 2), pl.ds(first, cols)]

    def o_block(z_, x_, c_, span):
        begin, size = span
        first = pl.multiple_of((z_ * 4 + x_ * 2 + c_) * cols + begin, 16)
        return wot.at[pl.ds(first, size), :]

    def o_span(item, k, direction, client):
        begin, size = 0, cols
        if item == 3 or (item == 1 and client):
            size = cols // 2
            begin = 0 if item == 3 else cols // 2
        if k == 3:
            size = size // 2
            begin += direction * size
        return begin, size

    def block(item, z_, c_, k, direction, client):
        if item == 0:
            return v_block(z_, xl, c_, None if k < 3 else direction)
        span = o_span(item, k, direction, client)
        if item == 3:
            return held.at[z_, pl.ds(*span), :]
        return o_block(z_, xl if item == 1 else 1 - xl, c_, span)

    def origin(direction, hops):
        return (z + (NZ - hops if direction == 0 else hops)) % NZ

    def remote(src, dst, sends, recvs, index, peer):
        return pltpu.make_async_remote_copy(
            src_ref=src, dst_ref=dst, send_sem=sends.at[0], recv_sem=recvs.at[index],
            device_id=peer, device_id_type=MESH,
        )

    def z_copy(direction, k, item, client):
        dst = block(item, origin(direction, k), core, k, direction, client)
        src = dst
        if k == 0 and item == 0:
            src = vt_own
        if k == 0 and item == 1:
            src = ot_own.at[pl.ds(*o_span(1, 0, direction, client)), :]
        return remote(src, dst, zs, zr, (direction, k, item), dev(z_next if direction == 0 else z_prev, xl, core))

    def z_arrival(direction, k, item, client):
        ref = block(item, origin(direction, k + 1), core, k, direction, client)
        return remote(ref, ref, zs, zr, (direction, k, item), dev(z_prev if direction == 0 else z_next, xl, core))

    def x_refs(index, x_):
        if index == 0:
            return o_block(z, x_, core, (0, cols))
        if index == 1:
            return v_block(z, x_, core, None)
        direction, k = (index - 2) // 4, (index - 2) % 4
        return v_block(origin(direction, k + 1), x_, core, None if k < 3 else direction)

    def x_copy(index):
        dst = x_refs(index, xl)
        return remote((ot_own, vt_own)[index] if index < 2 else dst, dst, xs, xr, index, dev(z, 1 - xl, core))

    def x_arrival(index):
        ref = x_refs(index, 1 - xl)
        return remote(ref, ref, xs, xr, index, dev(z, 1 - xl, core))

    def d_refs(index, c_, client):
        if index == 0:
            return o_block(z, xl, c_, (0, cols))
        if index == 1:
            return v_block(z, xl, c_, None)
        if index < 26:
            direction, k, item = (index - 2) // 12, (index - 2) // 3 % 4, (index - 2) % 3
            return block(item, origin(direction, k + 1), c_, k, direction, client)
        if index == 26:
            return o_block(z, 1 - xl, c_, (0, cols))
        if index == 27:
            return v_block(z, 1 - xl, c_, None)
        if index < 36:
            direction, k = (index - 28) // 4, (index - 28) % 4
            return v_block(origin(direction, k + 1), 1 - xl, c_, None if k < 3 else direction)
        direction, k = (index - 36) // 4, (index - 36) % 4
        return o_block(origin(direction, k + 1), xl, c_, o_span(3, k, direction, client))

    def d_group(index):
        if index in (1, 27):
            return 1
        if 2 <= index < 26 and (index - 2) % 3 == 0:
            return 2 + (index - 2) // 3 % 4
        if 28 <= index < 36:
            return 2 + (index - 28) % 4
        return 0

    def d_copy(index, client):
        dst = d_refs(index, core, client)
        src = (ot_own, vt_own)[index] if index < 2 else dst
        return remote(src, dst, ds_, dr, d_group(index), dev(z, xl, 1 - core))

    def d_arrivals(group):
        units = {0: 16, 1: 2, 5: 2}.get(group, 4)
        ref = wot.at[pl.ds(0, units * cols), :]
        return remote(ref, ref, ds_, dr, group, dev(z, xl, 1 - core))

    def all_sent(sends, ref):
        remote(ref, ref, sends, dr, 0, dev(z, xl, 1 - core)).wait_send()

    def lent_copy():
        return remote(ot_own.at[pl.ds(0, cols // 2), :], held.at[z], hs, hr, 0, outer)

    def lent_arrival():
        return remote(held.at[z], held.at[z], hs, hr, 0, outer)

    def back_copy(direction, k):
        zo = origin(direction, k + 1)
        span = o_span(3, k, direction, True)
        return remote(
            held.at[zo, pl.ds(*span), :], o_block(zo, 1 - xl, core, span), hs, hr, 1 + direction * 4 + k, outer
        )

    def back_arrival(direction, k):
        ref = o_block(origin(direction, k + 1), xl, core, o_span(3, k, direction, True))
        return remote(ref, ref, hs, hr, 1 + direction * 4 + k, outer)

    def value_pair(z_, x_):
        span = pl.ds(pl.multiple_of((z_ * 4 + x_ * 2) * cols, 2 * cols), 2 * cols)
        left = normed[:, span]
        for n in range(0, kv, 256):
            va_sum[:, n : n + 256] += lax.dot_general(
                left, wvt[n : n + 256, span], (((1,), (1,)), ((), ())), preferred_element_type=jnp.float32
            )

    def pairs_of(k, client):
        d_arrivals(2 + k).wait_recv()
        for direction in (0, 1):
            if 0 <= k < 3 or direction == 1:
                value_pair(origin(direction, k + 1), 0)
                value_pair(origin(direction, k + 1), 1)

    def begin(client):
        x_copy(0).start()
        x_copy(1).start()
        if client:
            lent_copy().start()
        for item in (0, 1) if client else (0,):
            for direction in (0, 1):
                z_copy(direction, 0, item, client).start()
        d_copy(0, client).start()
        d_copy(1, client).start()

    def z_step(direction, k, item, client):
        z_arrival(direction, k, item, client).wait_recv()
        if k < 3:
            z_copy(direction, k + 1, item, client).start()
        if item == 0:
            x_copy(2 + direction * 4 + k).start()
        if item == 3:
            back_copy(direction, k).start()
        else:
            d_copy(2 + direction * 12 + k * 3 + item, client).start()

    def x_step(k, client):
        for direction in (0, 1):
            x_arrival(2 + direction * 4 + k).wait_recv()
            d_copy(28 + direction * 4 + k, client).start()

    def last_waits(client):
        pairs_of(3, client)
        d_arrivals(0).wait_recv()

    def gather_client():
        x_arrival(0).wait_recv()
        for direction in (0, 1):
            z_copy(direction, 0, 2, True).start()
        d_copy(26, True).start()
        for k in range(4):
            for item in (0, 1):
                for direction in (0, 1):
                    z_step(direction, k, item, True)
            if k == 0:
                x_arrival(1).wait_recv()
                d_copy(27, True).start()
            else:
                x_step(k - 1, True)
            for direction in (0, 1):
                back_arrival(direction, k).wait_recv()
                d_copy(36 + direction * 4 + k, True).start()
            for direction in (0, 1):
                z_step(direction, k, 2, True)
            if k > 0:
                pairs_of(k - 2, True)
        pairs_of(2, True)
        x_step(3, True)
        last_waits(True)

    def gather_helper():
        lent_arrival().wait_recv()
        for direction in (0, 1):
            z_copy(direction, 0, 3, False).start()
        x_arrival(0).wait_recv()
        d_copy(26, False).start()
        for k in range(4):
            if k == 3:
                for item in (1, 2):
                    for direction in (0, 1):
                        z_copy(direction, 0, item, False).start()
            for item in (0, 3):
                for direction in (0, 1):
                    z_step(direction, k, item, False)
        x_arrival(1).wait_recv()
        d_copy(27, False).start()
        for k in range(4):
            for item in (1, 2):
                for direction in (0, 1):
                    z_step(direction, k, item, False)
            x_step(k, False)
            pairs_of(k - 1, False)
        last_waits(False)

    half_of = SECTIONS // 2

    @pl.when(sec >= half_of)
    def _():
        begin(True)

    @pl.when(sec < half_of)
    def _():
        begin(False)

    own = pl.ds(pl.multiple_of(shard * cols, cols), cols)
    wvt[:, own] = vt_own[...]
    wot[own, :] = ot_own[...]

    def prepare(b, carry):
        rows = pl.ds(pl.multiple_of(b * ROWS, ROWS), ROWS)
        hidden = act[rows, :].astype(jnp.float32)
        inverse = lax.rsqrt(jnp.mean(hidden * hidden, axis=-1, keepdims=True) + EPSILON)
        rms[rows, :] = jnp.broadcast_to(inverse, (ROWS, 128))
        normed[rows, :] = (hidden * inverse * gain[...]).astype(jnp.bfloat16)
        return carry

    local[0].wait()
    lax.fori_loop(0, BLOCKS, prepare, 0)
    local[4].wait()

    @pl.when(sec == SECTIONS - 1)
    def _():
        def masked(b, carry):
            rows = pl.ds(pl.multiple_of(b * ROWS, ROWS), ROWS)
            row_at = lax.broadcasted_iota(jnp.int32, (ROWS, LEN), 0) + b * ROWS
            col_at = lax.broadcasted_iota(jnp.int32, (ROWS, LEN), 1)
            kept = jnp.where(row_at == col_at, mask[...].astype(jnp.float32), 0.0)
            column = jnp.sum(kept, axis=-1, keepdims=True)
            c_in[b] = (top[rows, :].astype(jnp.float32) * column).astype(jnp.bfloat16)
            return carry

        lax.fori_loop(0, BLOCKS, masked, 0)

    local[1].wait()
    local[2].wait()
    local[3].wait()

    def lowered(b, carry):
        rows = pl.ds(pl.multiple_of(b * ROWS, ROWS), ROWS)
        store_low[rows, :] = store[rows, :].astype(jnp.bfloat16)
        return carry

    lax.fori_loop(0, store.shape[0] // ROWS, lowered, 0)
    va_sum[...] = jnp.zeros_like(va_sum)

    @pl.when(sec >= half_of)
    def _():
        gather_client()

    @pl.when(sec < half_of)
    def _():
        gather_helper()

    def value_path():
        va[...] = va_sum[...].astype(jnp.bfloat16)
        vlow[...] = lax.dot_general(
            va[...], vproj[...], (((1,), (1,)), ((), ())), preferred_element_type=jnp.float32
        )

    piece = width // PIECES

    def c_copy(b, n):
        span = pl.ds(n * piece, piece)
        group = [first <= n < last for first, last in GROUPS].index(True)
        return pltpu.make_async_remote_copy(
            src_ref=c_out.at[b, :, span], dst_ref=c_in.at[b, :, span], send_sem=cs.at[0], recv_sem=cr.at[b, group],
            device_id=(down, shard), device_id_type=MESH,
        )

    def arrived(b, group):
        first, last = GROUPS[group]
        ref = c_in.at[b, :, pl.ds(first * piece, (last - first) * piece)]
        pltpu.make_async_remote_copy(
            src_ref=ref, dst_ref=ref, send_sem=cs.at[0], recv_sem=cr.at[b, group],
            device_id=(up, shard), device_id_type=MESH,
        ).wait_recv()

    half_rows = gproj.shape[0] // 2

    def features():
        low = lax.dot_general(
            c_in[...].reshape(LEN, width), gproj[...], (((1,), (1,)), ((), ())), preferred_element_type=jnp.float32
        )
        feat[...] = lax.dot_general(
            low, vlow[...], (((0,), (0,)), ((), ())),
            precision=lax.Precision.HIGHEST, preferred_element_type=jnp.float32,
        )
        even = feat[pl.ds(0, half_rows, stride=2), :]
        odd = feat[pl.ds(1, half_rows, stride=2), :]
        packed = jnp.concatenate([even, odd], axis=1).astype(jnp.bfloat16)
        feat_own[...] = packed
        feats[shard] = packed

    @pl.when(sec < SECTIONS - 1)
    def _():
        value_path()

    def stage(b, top_layer):
        rows = pl.ds(pl.multiple_of(b * ROWS, ROWS), ROWS)
        grad_value = jnp.zeros((ROWS, kv), jnp.float32)
        for group, (first, last) in enumerate(GROUPS):
            if not top_layer:
                arrived(b, group)
            span = slice(first * piece, last * piece)
            grad_value += jnp.dot(c_in[b, :, span], wot[span, :], preferred_element_type=jnp.float32)
        grad_value = grad_value.astype(jnp.bfloat16)
        inverse = rms[rows, :][:, :1]
        total = jnp.sum(grad_value.astype(jnp.float32) * va_sum[rows, :], axis=-1, keepdims=True)
        back = (inverse * inverse) * (total / width)
        for n in range(PIECES):
            span = slice(n * piece, (n + 1) * piece)
            part = gain[:, span] * jnp.dot(grad_value, wvt[:, span], preferred_element_type=jnp.float32)
            hidden = act[rows, span].astype(jnp.float32)
            grad_input = inverse * part - hidden * back
            c_out[b, :, span] = (c_in[b, :, span].astype(jnp.float32) + grad_input).astype(jnp.bfloat16)
            c_copy(b, n).start()

    def stages(top_layer):
        def one(b, carry):
            stage(b, top_layer)
            return carry

        lax.fori_loop(0, BLOCKS, one, 0)

    def rows_of(units):
        return wot.at[pl.ds(0, units * cols // 2), :]

    def settle():
        @pl.when(sec >= half_of)
        def _():
            all_sent(zs, rows_of(35))
            all_sent(hs, rows_of(1))

        @pl.when(sec < half_of)
        def _():
            all_sent(zs, rows_of(49))
            all_sent(hs, rows_of(7))

        all_sent(xs, rows_of(18))
        all_sent(ds_, rows_of(64))

    @pl.when(sec < SECTIONS - 1)
    def _():
        settle()

    @pl.when(sec == 0)
    def _():
        def one(b, carry):
            for group in range(len(GROUPS)):
                arrived(b, group)
            return carry

        lax.fori_loop(0, BLOCKS, one, 0)

    @pl.when((sec > 0) & (sec < SECTIONS - 1))
    def _():
        stages(False)

    @pl.when(sec == SECTIONS - 1)
    def _():
        stages(True)

    @pl.when(sec == SECTIONS - 1)
    def _():
        value_path()

    features()

    def slot(p, c_):
        return ((z + NZ - p // 2) % NZ) * 4 + ((xl + p) % 2) * 2 + c_

    def f_copy(p):
        return pltpu.make_async_remote_copy(
            src_ref=feat_own, dst_ref=feats.at[shard], send_sem=fs.at[0], recv_sem=fr.at[p],
            device_id=dev((z + p // 2) % NZ, (xl + p) % 2, core), device_id_type=MESH,
        )

    def f_arrival(p):
        ref = feats.at[slot(p, core)]
        return pltpu.make_async_remote_copy(
            src_ref=ref, dst_ref=ref, send_sem=fs.at[0], recv_sem=fr.at[p],
            device_id=dev((z + NZ - p // 2) % NZ, (xl + p) % 2, core), device_id_type=MESH,
        )

    def g_copy(p):
        ref = feats.at[slot(p, core)]
        return pltpu.make_async_remote_copy(
            src_ref=feat_own if p == 0 else ref, dst_ref=ref, send_sem=gs.at[0], recv_sem=gr.at[0],
            device_id=dev(z, xl, 1 - core), device_id_type=MESH,
        )

    def g_arrivals():
        ref = feats.at[pl.ds(0, 2 * NZ)]
        return pltpu.make_async_remote_copy(
            src_ref=ref, dst_ref=ref, send_sem=gs.at[0], recv_sem=gr.at[0],
            device_id=dev(z, xl, 1 - core), device_id_type=MESH,
        )

    near = (0, 1, 7, 2, 6, 3, 5, 4)
    order = [2 * dz + dx for dz in near for dx in (0, 1)][1:]
    for p in reversed(order):
        f_copy(p).start()
    g_copy(0).start()
    for p in order:
        f_arrival(p).wait_recv()
        g_copy(p).start()
    g_arrivals().wait_recv()
    gens = feats.shape[0]
    for q in range(gens):
        feat_rows[q * half_rows : (q + 1) * half_rows, :] = feats[q].astype(jnp.float32)
    for i in range(half_rows):
        feat_all[:, i * 128 : (i + 1) * 128] = feat_rows[pl.ds(i, gens, stride=half_rows), :].astype(jnp.bfloat16)
    scores = lax.dot_general(
        feat_all[...], store_low[...], (((1,), (1,)), ((), ())), preferred_element_type=jnp.float32
    )
    gens_each = gens // SECTIONS
    for n in range(SECTIONS):
        part_out[n] = scores[n * gens_each : (n + 1) * gens_each, :]

    def p_copy(d):
        return pltpu.make_async_remote_copy(
            src_ref=part_out.at[(sec + d) % SECTIONS], dst_ref=part_in.at[d], send_sem=ps.at[0], recv_sem=pr.at[0],
            device_id=((sec + d) % SECTIONS, shard), device_id_type=MESH,
        )

    def p_arrivals():
        ref = part_in.at[pl.ds(1, SECTIONS - 1)]
        return pltpu.make_async_remote_copy(
            src_ref=ref, dst_ref=ref, send_sem=ps.at[0], recv_sem=pr.at[0],
            device_id=(down, shard), device_id_type=MESH,
        )

    for d in range(1, SECTIONS):
        p_copy(d).start()
    all_sent(fs, feats.at[pl.ds(0, 2 * NZ - 1)])
    all_sent(gs, feats.at[pl.ds(0, 2 * NZ)])

    @pl.when(sec > 0)
    def _():
        all_sent(cs, c_out)

    @pl.when(sec == SECTIONS - 1)
    def _():
        settle()

    total_scores = part_out[sec]
    p_arrivals().wait_recv()
    for d in range(1, SECTIONS):
        total_scores += part_in[d]
    p_arrivals().wait_send()
    out[...] = total_scores


def chain(act, top, mask, gain, v_own, o_own, vproj, gproj, store):
    tokens, width = act.shape
    kv = v_own.shape[1]
    proj = vproj.shape[0]
    examples = store.shape[0]
    gens = NZ * 4
    vmem = pl.BlockSpec(memory_space=pltpu.VMEM)
    hbm = pl.BlockSpec(memory_space=pltpu.HBM)
    dma = pltpu.SemaphoreType.DMA
    bf16, f32 = jnp.bfloat16, jnp.float32
    return pl.pallas_call(
        chain_kernel,
        out_shape=jax.ShapeDtypeStruct((gens // SECTIONS, examples), f32),
        in_specs=[hbm, hbm, vmem, vmem] + [hbm] * 5,
        out_specs=vmem,
        scratch_shapes=[
            pltpu.VMEM(act.shape, bf16),
            pltpu.VMEM(top.shape, bf16),
            pltpu.VMEM(vproj.shape, bf16),
            pltpu.VMEM(gproj.shape, bf16),
            pltpu.VMEM(store.shape, f32),
            pltpu.VMEM(v_own.shape, bf16),
            pltpu.VMEM(o_own.shape, bf16),
            pltpu.VMEM(v_own.shape[::-1], bf16),
            pltpu.VMEM(o_own.shape[::-1], bf16),
            pltpu.VMEM(store.shape, bf16),
            pltpu.VMEM((kv, width), bf16),
            pltpu.VMEM((width, kv), bf16),
            pltpu.VMEM((NZ, v_own.shape[0] // 2, kv), bf16),
            pltpu.VMEM((tokens, width), bf16),
            pltpu.VMEM((tokens, 128), f32),
            pltpu.VMEM((BLOCKS, ROWS, width), bf16),
            pltpu.VMEM((BLOCKS, ROWS, width), bf16),
            pltpu.VMEM((tokens, kv), f32),
            pltpu.VMEM((tokens, kv), bf16),
            pltpu.VMEM((tokens, proj), f32),
            pltpu.VMEM((proj, proj), f32),
            pltpu.VMEM((proj // 2, 2 * proj), bf16),
            pltpu.VMEM((gens, proj // 2, 2 * proj), bf16),
            pltpu.VMEM((gens * proj // 2, 2 * proj), f32),
            pltpu.VMEM((gens, proj * proj), bf16),
            pltpu.VMEM((SECTIONS, gens // SECTIONS, examples), f32),
            pltpu.VMEM((SECTIONS, gens // SECTIONS, examples), f32),
            dma((7,)),
            dma((1,)), dma((2, 4, 4)), dma((1,)), dma((10,)), dma((1,)), dma((6,)), dma((1,)), dma((9,)),
            dma((1,)), dma((BLOCKS, len(GROUPS))),
            dma((1,)), dma((2 * NZ,)), dma((1,)), dma((1,)), dma((1,)), dma((1,)),
        ],
        compiler_params=pltpu.CompilerParams(
            collective_id=0, has_side_effects=True, vmem_limit_bytes=60 * 1024 * 1024
        ),
        cost_estimate=pl.CostEstimate(flops=3 * 10**9, bytes_accessed=4 * 10**6, transcendentals=0),
    )(act, top, mask, gain, v_own, o_own, vproj, gproj, store)


def per_device(
    activations, top_grad, loss_mask, norm_gain, value_weight, output_weight, value_proj, grad_proj, store
):
    return chain(
        activations[0], top_grad, loss_mask.reshape(1, -1), norm_gain, value_weight[0], output_weight[0],
        value_proj[0].T, grad_proj[0].T, store[0],
    )


def solution(mesh):
    placed = (
        P("section", "shard", None),
        P("shard", None),
        P("shard"),
        P("section", None),
        P("section", "shard", None),
        P("section", None, "shard"),
        P("section", None, None),
        P("section", None, None),
        P("section", "shard", None),
    )
    return jax.shard_map(
        per_device, mesh=mesh, in_specs=placed, out_specs=P("section", "shard"), check_vma=False
    )
```

```python
import jax
import jax.numpy as jnp
from jax import lax
from jax.experimental import pallas as pl
from jax.experimental.pallas import tpu as pltpu
from jax.sharding import PartitionSpec as P

LEN = 96
EPSILON = 1e-05
MESH = pl.DeviceIdType.MESH
NZ = 8
SECTIONS = 8
ROWS = 16
BLOCKS = LEN // ROWS
PIECES = 4
GROUPS = ((0, 3), (3, 4))


def chain_kernel(
    act_hbm, top_hbm, mask, gain, v_hbm, o_hbm, vproj_hbm, gproj_hbm, store_hbm,
    out,
    act, top, vproj, gproj, store, v_raw, o_raw, vt_own, ot_own, store_low,
    wvt, wot, held, normed, rms, c_in, c_out, va_sum, va, vlow,
    feat, feat_own, feats, feat_rows, feat_all, part_out, part_in,
    ls, zs, zr, xs, xr, ds_, dr, hs, hr, cs, cr, fs, fr, gs, gr, ps, pr,
):
    sec = lax.axis_index("section")
    shard = lax.axis_index("shard")
    z = shard // 4
    xl = (shard // 2) % 2
    core = shard % 2
    width = act.shape[1]
    kv = wot.shape[1]
    cols = vt_own.shape[1]

    def dev(z_, x_, c_):
        return (sec, z_ * 4 + x_ * 2 + c_)

    z_next = (z + 1) % NZ
    z_prev = (z + NZ - 1) % NZ
    up = (sec + 1) % SECTIONS
    down = (sec + SECTIONS - 1) % SECTIONS
    own_v = pltpu.make_async_copy(v_hbm, v_raw, ls.at[0])
    own_o = pltpu.make_async_copy(o_hbm, o_raw, ls.at[1])
    own_v.start()
    own_o.start()
    barrier = pltpu.get_barrier_semaphore()
    peers = [dev((z + p // 2) % NZ, (xl + p) % 2, core) for p in range(1, 2 * NZ)]
    outer = ((sec + SECTIONS // 2) % SECTIONS, z * 4 + (1 - xl) * 2 + core)
    peers.append(outer)
    peers.append(dev(z, xl, 1 - core))
    peers.extend([((sec + d) % SECTIONS, shard) for d in range(1, SECTIONS)])
    for peer in peers:
        pl.semaphore_signal(barrier, inc=1, device_id=peer, device_id_type=MESH)
    local = [
        pltpu.make_async_copy(source, target, ls.at[2 + n])
        for n, (source, target) in enumerate(
            ((act_hbm, act), (gproj_hbm, gproj), (vproj_hbm, vproj), (store_hbm, store), (top_hbm, top))
        )
    ]
    for copy in local:
        copy.start()
    own_o.wait()
    ot_own[...] = o_raw[...].T
    own_v.wait()
    vt_own[...] = v_raw[...].T
    pl.semaphore_wait(barrier, len(peers))

    def v_block(z_, x_, c_, half):
        first = pl.multiple_of((z_ * 4 + x_ * 2 + c_) * cols, cols)
        if half is None:
            return wvt.at[:, pl.ds(first, cols)]
        return wvt.at[pl.ds(half * (kv // 2), kv // 2), pl.ds(first, cols)]

    def v_rows(z_, x_, c_, begin, size):
        first = pl.multiple_of((z_ * 4 + x_ * 2 + c_) * cols, cols)
        return wvt.at[pl.ds(begin, size), pl.ds(first, cols)]

    def o_block(z_, x_, c_, span):
        begin, size = span
        first = pl.multiple_of((z_ * 4 + x_ * 2 + c_) * cols + begin, 16)
        return wot.at[pl.ds(first, size), :]

    lent = cols * 3 // 4
    side = kv // 8

    def o_span(item, k, direction, client):
        begin, size = 0, cols
        if item == 3:
            size = lent
        if item == 1 and client:
            begin, size = lent, cols - lent
        if k == 3:
            size = size // 2
            begin += direction * size
        return begin, size

    def block(item, z_, c_, k, direction, client):
        if item == 0:
            return v_block(z_, xl, c_, None if k < 3 else direction)
        if item == 4:
            return v_rows(z_, 1 - xl, c_, *((0, side) if k < 3 else (direction * side // 2, side // 2)))
        span = o_span(item, k, direction, client)
        if item == 3:
            return held.at[z_, pl.ds(*span), :]
        return o_block(z_, xl if item == 1 else 1 - xl, c_, span)

    def origin(direction, hops):
        return (z + (NZ - hops if direction == 0 else hops)) % NZ

    def remote(src, dst, sends, recvs, index, peer):
        return pltpu.make_async_remote_copy(
            src_ref=src, dst_ref=dst, send_sem=sends.at[0], recv_sem=recvs.at[index],
            device_id=peer, device_id_type=MESH,
        )

    def z_copy(direction, k, item, client):
        dst = block(item, origin(direction, k), core, k, direction, client)
        src = dst
        if k == 0 and item == 0:
            src = vt_own
        if k == 0 and item == 1:
            src = ot_own.at[pl.ds(*o_span(1, 0, direction, client)), :]
        return remote(src, dst, zs, zr, (direction, k, item), dev(z_next if direction == 0 else z_prev, xl, core))

    def z_arrival(direction, k, item, client):
        ref = block(item, origin(direction, k + 1), core, k, direction, client)
        return remote(ref, ref, zs, zr, (direction, k, item), dev(z_prev if direction == 0 else z_next, xl, core))

    def x_forward(z_, x_, c_, direction, k, client):
        begin, end = (0, kv) if k < 3 else (direction * (kv // 2), (direction + 1) * (kv // 2))
        if client:
            begin = max(begin, side)
        return v_rows(z_, x_, c_, begin, end - begin)

    def x_refs(index, x_, client):
        if index == 0:
            return o_block(z, x_, core, (0, cols))
        if index == 1:
            return v_block(z, x_, core, None)
        direction, k = (index - 2) // 4, (index - 2) % 4
        return x_forward(origin(direction, k + 1), x_, core, direction, k, client)

    def x_copy(index, client):
        dst = x_refs(index, xl, client)
        return remote((ot_own, vt_own)[index] if index < 2 else dst, dst, xs, xr, index, dev(z, 1 - xl, core))

    def x_arrival(index, client):
        ref = x_refs(index, 1 - xl, client)
        return remote(ref, ref, xs, xr, index, dev(z, 1 - xl, core))

    def d_refs(index, c_, client):
        if index == 0:
            return o_block(z, xl, c_, (0, cols))
        if index == 1:
            return v_block(z, xl, c_, None)
        if index < 26:
            direction, k, item = (index - 2) // 12, (index - 2) // 3 % 4, (index - 2) % 3
            return block(item, origin(direction, k + 1), c_, k, direction, client)
        if index == 26:
            return o_block(z, 1 - xl, c_, (0, cols))
        if index == 27:
            return v_block(z, 1 - xl, c_, None)
        if index < 36:
            direction, k = (index - 28) // 4, (index - 28) % 4
            return x_forward(origin(direction, k + 1), 1 - xl, c_, direction, k, client)
        if index >= 44:
            direction, k = (index - 44) // 4, (index - 44) % 4
            return block(4, origin(direction, k + 1), c_, k, direction, client)
        direction, k = (index - 36) // 4, (index - 36) % 4
        return o_block(origin(direction, k + 1), xl, c_, o_span(3, k, direction, client))

    def d_group(index):
        if index in (1, 27):
            return 1
        if 2 <= index < 26 and (index - 2) % 3 == 0:
            return 2 + (index - 2) // 3 % 4
        if 28 <= index < 36:
            return 2 + (index - 28) % 4
        if index >= 44:
            return 2 + (index - 44) % 4
        return 0

    def d_copy(index, client):
        dst = d_refs(index, core, client)
        src = (ot_own, vt_own)[index] if index < 2 else dst
        return remote(src, dst, ds_, dr, d_group(index), dev(z, xl, 1 - core))

    def d_arrivals(group):
        units = {0: 16, 1: 2, 5: 2}.get(group, 4)
        ref = wot.at[pl.ds(0, units * cols), :]
        return remote(ref, ref, ds_, dr, group, dev(z, xl, 1 - core))

    def all_sent(sends, ref):
        remote(ref, ref, sends, dr, 0, dev(z, xl, 1 - core)).wait_send()

    def lent_copy():
        return remote(ot_own.at[pl.ds(0, lent), :], held.at[z], hs, hr, 0, outer)

    def lent_arrival():
        return remote(held.at[z], held.at[z], hs, hr, 0, outer)

    def back_copy(direction, k):
        zo = origin(direction, k + 1)
        span = o_span(3, k, direction, True)
        return remote(
            held.at[zo, pl.ds(*span), :], o_block(zo, 1 - xl, core, span), hs, hr, 1 + direction * 4 + k, outer
        )

    def back_arrival(direction, k):
        ref = o_block(origin(direction, k + 1), xl, core, o_span(3, k, direction, True))
        return remote(ref, ref, hs, hr, 1 + direction * 4 + k, outer)

    def value_pair(z_, x_):
        span = pl.ds(pl.multiple_of((z_ * 4 + x_ * 2) * cols, 2 * cols), 2 * cols)
        left = normed[:, span]
        for n in range(0, kv, 256):
            va_sum[:, n : n + 256] += lax.dot_general(
                left, wvt[n : n + 256, span], (((1,), (1,)), ((), ())), preferred_element_type=jnp.float32
            )

    def pairs_of(k, client):
        d_arrivals(2 + k).wait_recv()
        for direction in (0, 1):
            if 0 <= k < 3 or direction == 1:
                value_pair(origin(direction, k + 1), 0)
                value_pair(origin(direction, k + 1), 1)

    def begin(client):
        x_copy(0, client).start()
        x_copy(1, client).start()
        if client:
            lent_copy().start()
        for item in (0, 1) if client else (0,):
            for direction in (0, 1):
                z_copy(direction, 0, item, client).start()
        d_copy(0, client).start()
        d_copy(1, client).start()

    def z_step(direction, k, item, client):
        z_arrival(direction, k, item, client).wait_recv()
        if k < 3:
            z_copy(direction, k + 1, item, client).start()
        if item == 0:
            x_copy(2 + direction * 4 + k, client).start()
        if item == 3:
            back_copy(direction, k).start()
        elif item == 4:
            d_copy(44 + direction * 4 + k, client).start()
        else:
            d_copy(2 + direction * 12 + k * 3 + item, client).start()

    def x_step(k, client):
        for direction in (0, 1):
            x_arrival(2 + direction * 4 + k, client).wait_recv()
            d_copy(28 + direction * 4 + k, client).start()

    def last_waits(client):
        pairs_of(3, client)
        d_arrivals(0).wait_recv()

    def gather_client():
        x_arrival(0, True).wait_recv()
        for direction in (0, 1):
            z_copy(direction, 0, 2, True).start()
        d_copy(26, True).start()
        for k in range(4):
            for item in (0, 1):
                for direction in (0, 1):
                    z_step(direction, k, item, True)
            if k == 0:
                x_arrival(1, True).wait_recv()
                d_copy(27, True).start()
                for direction in (0, 1):
                    z_copy(direction, 0, 4, True).start()
            else:
                x_step(k - 1, True)
            for direction in (0, 1):
                back_arrival(direction, k).wait_recv()
                d_copy(36 + direction * 4 + k, True).start()
            for item in (2, 4):
                for direction in (0, 1):
                    z_step(direction, k, item, True)
            if k > 0:
                pairs_of(k - 2, True)
        pairs_of(2, True)
        x_step(3, True)
        last_waits(True)

    def gather_helper():
        lent_arrival().wait_recv()
        for direction in (0, 1):
            z_copy(direction, 0, 3, False).start()
        x_arrival(0, False).wait_recv()
        d_copy(26, False).start()
        for k in range(4):
            if k == 3:
                for item in (1, 2):
                    for direction in (0, 1):
                        z_copy(direction, 0, item, False).start()
            for item in (0, 3):
                for direction in (0, 1):
                    z_step(direction, k, item, False)
        x_arrival(1, False).wait_recv()
        d_copy(27, False).start()
        for k in range(4):
            for item in (1, 2):
                for direction in (0, 1):
                    z_step(direction, k, item, False)
            x_step(k, False)
            pairs_of(k - 1, False)
        last_waits(False)

    half_of = SECTIONS // 2

    @pl.when(sec >= half_of)
    def _():
        begin(True)

    @pl.when(sec < half_of)
    def _():
        begin(False)

    own = pl.ds(pl.multiple_of(shard * cols, cols), cols)
    wvt[:, own] = vt_own[...]
    wot[own, :] = ot_own[...]

    def prepare(b, carry):
        rows = pl.ds(pl.multiple_of(b * ROWS, ROWS), ROWS)
        hidden = act[rows, :].astype(jnp.float32)
        inverse = lax.rsqrt(jnp.mean(hidden * hidden, axis=-1, keepdims=True) + EPSILON)
        rms[rows, :] = jnp.broadcast_to(inverse, (ROWS, 128))
        normed[rows, :] = (hidden * inverse * gain[...]).astype(jnp.bfloat16)
        return carry

    local[0].wait()
    lax.fori_loop(0, BLOCKS, prepare, 0)
    local[4].wait()

    @pl.when(sec == SECTIONS - 1)
    def _():
        def masked(b, carry):
            rows = pl.ds(pl.multiple_of(b * ROWS, ROWS), ROWS)
            row_at = lax.broadcasted_iota(jnp.int32, (ROWS, LEN), 0) + b * ROWS
            col_at = lax.broadcasted_iota(jnp.int32, (ROWS, LEN), 1)
            kept = jnp.where(row_at == col_at, mask[...].astype(jnp.float32), 0.0)
            column = jnp.sum(kept, axis=-1, keepdims=True)
            c_in[b] = (top[rows, :].astype(jnp.float32) * column).astype(jnp.bfloat16)
            return carry

        lax.fori_loop(0, BLOCKS, masked, 0)

    local[1].wait()
    local[2].wait()
    local[3].wait()

    def lowered(b, carry):
        rows = pl.ds(pl.multiple_of(b * ROWS, ROWS), ROWS)
        store_low[rows, :] = store[rows, :].astype(jnp.bfloat16)
        return carry

    lax.fori_loop(0, store.shape[0] // ROWS, lowered, 0)
    va_sum[...] = jnp.zeros_like(va_sum)

    @pl.when(sec >= half_of)
    def _():
        gather_client()

    @pl.when(sec < half_of)
    def _():
        gather_helper()

    def value_path():
        va[...] = va_sum[...].astype(jnp.bfloat16)
        vlow[...] = lax.dot_general(
            va[...], vproj[...], (((1,), (1,)), ((), ())), preferred_element_type=jnp.float32
        )

    piece = width // PIECES

    def c_copy(b, n):
        span = pl.ds(n * piece, piece)
        group = [first <= n < last for first, last in GROUPS].index(True)
        return pltpu.make_async_remote_copy(
            src_ref=c_out.at[b, :, span], dst_ref=c_in.at[b, :, span], send_sem=cs.at[0], recv_sem=cr.at[b, group],
            device_id=(down, shard), device_id_type=MESH,
        )

    def arrived(b, group):
        first, last = GROUPS[group]
        ref = c_in.at[b, :, pl.ds(first * piece, (last - first) * piece)]
        pltpu.make_async_remote_copy(
            src_ref=ref, dst_ref=ref, send_sem=cs.at[0], recv_sem=cr.at[b, group],
            device_id=(up, shard), device_id_type=MESH,
        ).wait_recv()

    half_rows = gproj.shape[0] // 2

    def features():
        low = lax.dot_general(
            c_in[...].reshape(LEN, width), gproj[...], (((1,), (1,)), ((), ())), preferred_element_type=jnp.float32
        )
        feat[...] = lax.dot_general(
            low, vlow[...], (((0,), (0,)), ((), ())),
            precision=lax.Precision.HIGHEST, preferred_element_type=jnp.float32,
        )
        even = feat[pl.ds(0, half_rows, stride=2), :]
        odd = feat[pl.ds(1, half_rows, stride=2), :]
        packed = jnp.concatenate([even, odd], axis=1).astype(jnp.bfloat16)
        feat_own[...] = packed
        feats[shard] = packed

    @pl.when(sec < SECTIONS - 1)
    def _():
        value_path()

    def stage(b, top_layer, eager):
        rows = pl.ds(pl.multiple_of(b * ROWS, ROWS), ROWS)
        if eager:
            grad_value = jnp.zeros((ROWS, kv), jnp.float32)
            for group, (first, last) in enumerate(GROUPS):
                arrived(b, group)
                span = slice(first * piece, last * piece)
                grad_value += jnp.dot(c_in[b, :, span], wot[span, :], preferred_element_type=jnp.float32)
        else:
            if not top_layer:
                for group in range(len(GROUPS)):
                    arrived(b, group)
            grad_value = jnp.dot(c_in[b], wot[...], preferred_element_type=jnp.float32)
        grad_value = grad_value.astype(jnp.bfloat16)
        inverse = rms[rows, :][:, :1]
        total = jnp.sum(grad_value.astype(jnp.float32) * va_sum[rows, :], axis=-1, keepdims=True)
        back = (inverse * inverse) * (total / width)
        for n in range(PIECES):
            span = slice(n * piece, (n + 1) * piece)
            part = gain[:, span] * jnp.dot(grad_value, wvt[:, span], preferred_element_type=jnp.float32)
            hidden = act[rows, span].astype(jnp.float32)
            grad_input = inverse * part - hidden * back
            c_out[b, :, span] = (c_in[b, :, span].astype(jnp.float32) + grad_input).astype(jnp.bfloat16)
            c_copy(b, n).start()

    def stages(top_layer):
        def one(b, carry):
            stage(b, top_layer, False)
            return carry

        if not top_layer:
            stage(0, False, True)
        lax.fori_loop(0 if top_layer else 1, BLOCKS, one, 0)

    def rows_of(count):
        return wot.at[pl.ds(0, count), :]

    def settle():
        wide = 7 * cols
        moved = side * cols // kv

        @pl.when(sec >= half_of)
        def _():
            all_sent(zs, rows_of(2 * wide + 7 * (cols - lent) + 7 * moved))
            all_sent(hs, rows_of(lent))
            all_sent(xs, rows_of(2 * cols + wide - 7 * moved))

        @pl.when(sec < half_of)
        def _():
            all_sent(zs, rows_of(3 * wide + 7 * lent))
            all_sent(hs, rows_of(7 * lent))
            all_sent(xs, rows_of(2 * cols + wide))

        all_sent(ds_, rows_of(4 * wide + 4 * cols))

    @pl.when(sec < SECTIONS - 1)
    def _():
        settle()

    @pl.when(sec == 0)
    def _():
        def one(b, carry):
            for group in range(len(GROUPS)):
                arrived(b, group)
            return carry

        lax.fori_loop(0, BLOCKS, one, 0)

    @pl.when((sec > 0) & (sec < SECTIONS - 1))
    def _():
        stages(False)

    @pl.when(sec == SECTIONS - 1)
    def _():
        stages(True)

    @pl.when(sec == SECTIONS - 1)
    def _():
        value_path()

    features()

    def slot(p, c_):
        return ((z + NZ - p // 2) % NZ) * 4 + ((xl + p) % 2) * 2 + c_

    def f_copy(p):
        return pltpu.make_async_remote_copy(
            src_ref=feat_own, dst_ref=feats.at[shard], send_sem=fs.at[0], recv_sem=fr.at[p],
            device_id=dev((z + p // 2) % NZ, (xl + p) % 2, core), device_id_type=MESH,
        )

    def f_arrival(p):
        ref = feats.at[slot(p, core)]
        return pltpu.make_async_remote_copy(
            src_ref=ref, dst_ref=ref, send_sem=fs.at[0], recv_sem=fr.at[p],
            device_id=dev((z + NZ - p // 2) % NZ, (xl + p) % 2, core), device_id_type=MESH,
        )

    def g_copy(p):
        ref = feats.at[slot(p, core)]
        return pltpu.make_async_remote_copy(
            src_ref=feat_own if p == 0 else ref, dst_ref=ref, send_sem=gs.at[0], recv_sem=gr.at[0],
            device_id=dev(z, xl, 1 - core), device_id_type=MESH,
        )

    def g_arrivals():
        ref = feats.at[pl.ds(0, 2 * NZ)]
        return pltpu.make_async_remote_copy(
            src_ref=ref, dst_ref=ref, send_sem=gs.at[0], recv_sem=gr.at[0],
            device_id=dev(z, xl, 1 - core), device_id_type=MESH,
        )

    near = (0, 1, 7, 2, 6, 3, 5, 4)
    order = [2 * dz + dx for dz in near for dx in (0, 1)][1:]
    for p in reversed(order):
        f_copy(p).start()
    g_copy(0).start()
    for p in order:
        f_arrival(p).wait_recv()
        g_copy(p).start()
    g_arrivals().wait_recv()
    gens = feats.shape[0]
    for q in range(gens):
        feat_rows[q * half_rows : (q + 1) * half_rows, :] = feats[q].astype(jnp.float32)
    for i in range(half_rows):
        feat_all[:, i * 128 : (i + 1) * 128] = feat_rows[pl.ds(i, gens, stride=half_rows), :].astype(jnp.bfloat16)
    scores = lax.dot_general(
        feat_all[...], store_low[...], (((1,), (1,)), ((), ())), preferred_element_type=jnp.float32
    )
    gens_each = gens // SECTIONS
    for n in range(SECTIONS):
        part_out[n] = scores[n * gens_each : (n + 1) * gens_each, :]

    def p_copy(d):
        return pltpu.make_async_remote_copy(
            src_ref=part_out.at[(sec + d) % SECTIONS], dst_ref=part_in.at[d], send_sem=ps.at[0], recv_sem=pr.at[0],
            device_id=((sec + d) % SECTIONS, shard), device_id_type=MESH,
        )

    def p_arrivals():
        ref = part_in.at[pl.ds(1, SECTIONS - 1)]
        return pltpu.make_async_remote_copy(
            src_ref=ref, dst_ref=ref, send_sem=ps.at[0], recv_sem=pr.at[0],
            device_id=(down, shard), device_id_type=MESH,
        )

    for d in range(1, SECTIONS):
        p_copy(d).start()
    all_sent(fs, feats.at[pl.ds(0, 2 * NZ - 1)])
    all_sent(gs, feats.at[pl.ds(0, 2 * NZ)])

    @pl.when(sec > 0)
    def _():
        all_sent(cs, c_out)

    @pl.when(sec == SECTIONS - 1)
    def _():
        settle()

    part_in[0] = part_out[sec]
    p_arrivals().wait_send()
    p_arrivals().wait_recv()
    out[...] = part_in[...]


def chain(act, top, mask, gain, v_own, o_own, vproj, gproj, store):
    tokens, width = act.shape
    kv = v_own.shape[1]
    proj = vproj.shape[0]
    examples = store.shape[0]
    gens = NZ * 4
    vmem = pl.BlockSpec(memory_space=pltpu.VMEM)
    hbm = pl.BlockSpec(memory_space=pltpu.HBM)
    dma = pltpu.SemaphoreType.DMA
    bf16, f32 = jnp.bfloat16, jnp.float32
    return pl.pallas_call(
        chain_kernel,
        out_shape=jax.ShapeDtypeStruct((SECTIONS, gens // SECTIONS, examples), f32),
        in_specs=[hbm, hbm, vmem, vmem] + [hbm] * 5,
        out_specs=vmem,
        scratch_shapes=[
            pltpu.VMEM(act.shape, bf16),
            pltpu.VMEM(top.shape, bf16),
            pltpu.VMEM(vproj.shape, bf16),
            pltpu.VMEM(gproj.shape, bf16),
            pltpu.VMEM(store.shape, f32),
            pltpu.VMEM(v_own.shape, bf16),
            pltpu.VMEM(o_own.shape, bf16),
            pltpu.VMEM(v_own.shape[::-1], bf16),
            pltpu.VMEM(o_own.shape[::-1], bf16),
            pltpu.VMEM(store.shape, bf16),
            pltpu.VMEM((kv, width), bf16),
            pltpu.VMEM((width, kv), bf16),
            pltpu.VMEM((NZ, v_own.shape[0] * 3 // 4, kv), bf16),
            pltpu.VMEM((tokens, width), bf16),
            pltpu.VMEM((tokens, 128), f32),
            pltpu.VMEM((BLOCKS, ROWS, width), bf16),
            pltpu.VMEM((BLOCKS, ROWS, width), bf16),
            pltpu.VMEM((tokens, kv), f32),
            pltpu.VMEM((tokens, kv), bf16),
            pltpu.VMEM((tokens, proj), f32),
            pltpu.VMEM((proj, proj), f32),
            pltpu.VMEM((proj // 2, 2 * proj), bf16),
            pltpu.VMEM((gens, proj // 2, 2 * proj), bf16),
            pltpu.VMEM((gens * proj // 2, 2 * proj), f32),
            pltpu.VMEM((gens, proj * proj), bf16),
            pltpu.VMEM((SECTIONS, gens // SECTIONS, examples), f32),
            pltpu.VMEM((SECTIONS, gens // SECTIONS, examples), f32),
            dma((7,)),
            dma((1,)), dma((2, 4, 5)), dma((1,)), dma((10,)), dma((1,)), dma((6,)), dma((1,)), dma((9,)),
            dma((1,)), dma((BLOCKS, len(GROUPS))),
            dma((1,)), dma((2 * NZ,)), dma((1,)), dma((1,)), dma((1,)), dma((1,)),
        ],
        compiler_params=pltpu.CompilerParams(
            collective_id=0, has_side_effects=True, vmem_limit_bytes=60 * 1024 * 1024
        ),
        cost_estimate=pl.CostEstimate(flops=3 * 10**9, bytes_accessed=4 * 10**6, transcendentals=0),
    )(act, top, mask, gain, v_own, o_own, vproj, gproj, store)


def per_device(
    activations, top_grad, loss_mask, norm_gain, value_weight, output_weight, value_proj, grad_proj, store
):
    parts = chain(
        activations[0], top_grad, loss_mask.reshape(1, -1), norm_gain, value_weight[0], output_weight[0],
        value_proj[0].T, grad_proj[0].T, store[0],
    )
    return parts.sum(axis=0)


def solution(mesh):
    placed = (
        P("section", "shard", None),
        P("shard", None),
        P("shard"),
        P("section", None),
        P("section", "shard", None),
        P("section", None, "shard"),
        P("section", None, None),
        P("section", None, None),
        P("section", "shard", None),
    )
    return jax.shard_map(
        per_device, mesh=mesh, in_specs=placed, out_specs=P("section", "shard"), check_vma=False
    )
```

```python
import jax
import jax.numpy as jnp
from jax import lax
from jax.experimental import pallas as pl
from jax.experimental.pallas import tpu as pltpu
from jax.sharding import PartitionSpec as P

LEN = 96
EPSILON = 1e-05
MESH = pl.DeviceIdType.MESH
NZ = 8
SECTIONS = 8
ROWS = 16
BLOCKS = LEN // ROWS
PIECES = 4
GROUPS = ((0, 3), (3, 4))


def chain_kernel(
    act_hbm, top_hbm, mask, gain, v_hbm, o_hbm, vproj_hbm, gproj_hbm, store_hbm,
    out,
    act, top, vproj, gproj, store, v_raw, o_raw, vt_own, ot_own, store_low,
    wvt, wot, held, normed, rms, c_in, c_out, va_sum, va, vlow,
    feat, feat_own, gproj_in, vlow_in, feat_in, feats, feat_rows, feat_all, part_out, part_in,
    ls, zs, zr, xs, xr, ds_, dr, hs, hr, cs, cr, fs, fr, gs, gr, ps, pr, es, er, ns,
):
    sec = lax.axis_index("section")
    shard = lax.axis_index("shard")
    z = shard // 4
    xl = (shard // 2) % 2
    core = shard % 2
    width = act.shape[1]
    kv = wot.shape[1]
    cols = vt_own.shape[1]

    def dev(z_, x_, c_):
        return (sec, z_ * 4 + x_ * 2 + c_)

    z_next = (z + 1) % NZ
    z_prev = (z + NZ - 1) % NZ
    up = (sec + 1) % SECTIONS
    down = (sec + SECTIONS - 1) % SECTIONS
    own_v = pltpu.make_async_copy(v_hbm, v_raw, ls.at[0])
    own_o = pltpu.make_async_copy(o_hbm, o_raw, ls.at[1])
    own_v.start()
    own_o.start()
    barrier = pltpu.get_barrier_semaphore()
    peers = [dev((z + p // 2) % NZ, (xl + p) % 2, core) for p in range(1, 2 * NZ)]
    outer = ((sec + SECTIONS // 2) % SECTIONS, z * 4 + (1 - xl) * 2 + core)
    peers.append(outer)
    peers.append(dev(z, xl, 1 - core))
    peers.extend([((sec + d) % SECTIONS, shard) for d in range(1, SECTIONS)])
    for peer in peers:
        pl.semaphore_signal(barrier, inc=1, device_id=peer, device_id_type=MESH)

    @pl.when(sec == 0)
    def _():
        for p in range(1, 2 * NZ):
            _, place = dev((z + p // 2) % NZ, (xl + p) % 2, core)
            pl.semaphore_signal(barrier, inc=1, device_id=(1, place), device_id_type=MESH)

    local = [
        pltpu.make_async_copy(source, target, ls.at[2 + n])
        for n, (source, target) in enumerate(
            ((act_hbm, act), (gproj_hbm, gproj), (vproj_hbm, vproj), (store_hbm, store), (top_hbm, top))
        )
    ]
    for copy in local:
        copy.start()
    own_o.wait()
    ot_own[...] = o_raw[...].T
    own_v.wait()
    vt_own[...] = v_raw[...].T

    @pl.when(sec == 1)
    def _():
        pl.semaphore_wait(barrier, len(peers) + 2 * NZ - 1)

    @pl.when(sec != 1)
    def _():
        pl.semaphore_wait(barrier, len(peers))

    def ahead(n):
        return pltpu.make_async_remote_copy(
            src_ref=(gproj, vlow)[n], dst_ref=(gproj_in, vlow_in)[n], send_sem=es.at[n], recv_sem=er.at[n],
            device_id=(up, shard), device_id_type=MESH,
        )


    def v_block(z_, x_, c_, half):
        first = pl.multiple_of((z_ * 4 + x_ * 2 + c_) * cols, cols)
        if half is None:
            return wvt.at[:, pl.ds(first, cols)]
        return wvt.at[pl.ds(half * (kv // 2), kv // 2), pl.ds(first, cols)]

    def v_rows(z_, x_, c_, begin, size):
        first = pl.multiple_of((z_ * 4 + x_ * 2 + c_) * cols, cols)
        return wvt.at[pl.ds(begin, size), pl.ds(first, cols)]

    def o_block(z_, x_, c_, span):
        begin, size = span
        first = pl.multiple_of((z_ * 4 + x_ * 2 + c_) * cols + begin, 16)
        return wot.at[pl.ds(first, size), :]

    lent = cols * 3 // 4
    side = kv // 8

    def o_span(item, k, direction, client):
        begin, size = 0, cols
        if item == 3:
            size = lent
        if item == 1 and client:
            begin, size = lent, cols - lent
        if k == 3:
            size = size // 2
            begin += direction * size
        return begin, size

    def block(item, z_, c_, k, direction, client):
        if item == 0:
            return v_block(z_, xl, c_, None if k < 3 else direction)
        if item == 4:
            return v_rows(z_, 1 - xl, c_, *((0, side) if k < 3 else (direction * side // 2, side // 2)))
        span = o_span(item, k, direction, client)
        if item == 3:
            return held.at[z_, pl.ds(*span), :]
        return o_block(z_, xl if item == 1 else 1 - xl, c_, span)

    def origin(direction, hops):
        return (z + (NZ - hops if direction == 0 else hops)) % NZ

    def remote(src, dst, sends, recvs, index, peer):
        return pltpu.make_async_remote_copy(
            src_ref=src, dst_ref=dst, send_sem=sends.at[0], recv_sem=recvs.at[index],
            device_id=peer, device_id_type=MESH,
        )

    def z_copy(direction, k, item, client):
        dst = block(item, origin(direction, k), core, k, direction, client)
        src = dst
        if k == 0 and item == 0:
            src = vt_own
        if k == 0 and item == 1:
            src = ot_own.at[pl.ds(*o_span(1, 0, direction, client)), :]
        return remote(src, dst, zs, zr, (direction, k, item), dev(z_next if direction == 0 else z_prev, xl, core))

    def z_arrival(direction, k, item, client):
        ref = block(item, origin(direction, k + 1), core, k, direction, client)
        return remote(ref, ref, zs, zr, (direction, k, item), dev(z_prev if direction == 0 else z_next, xl, core))

    def x_forward(z_, x_, c_, direction, k, client):
        begin, end = (0, kv) if k < 3 else (direction * (kv // 2), (direction + 1) * (kv // 2))
        if client:
            begin = max(begin, side)
        return v_rows(z_, x_, c_, begin, end - begin)

    def x_refs(index, x_, client):
        if index == 0:
            return o_block(z, x_, core, (0, cols))
        if index == 1:
            return v_block(z, x_, core, None)
        direction, k = (index - 2) // 4, (index - 2) % 4
        return x_forward(origin(direction, k + 1), x_, core, direction, k, client)

    def x_copy(index, client):
        dst = x_refs(index, xl, client)
        return remote((ot_own, vt_own)[index] if index < 2 else dst, dst, xs, xr, index, dev(z, 1 - xl, core))

    def x_arrival(index, client):
        ref = x_refs(index, 1 - xl, client)
        return remote(ref, ref, xs, xr, index, dev(z, 1 - xl, core))

    def d_refs(index, c_, client):
        if index == 0:
            return o_block(z, xl, c_, (0, cols))
        if index == 1:
            return v_block(z, xl, c_, None)
        if index < 26:
            direction, k, item = (index - 2) // 12, (index - 2) // 3 % 4, (index - 2) % 3
            return block(item, origin(direction, k + 1), c_, k, direction, client)
        if index == 26:
            return o_block(z, 1 - xl, c_, (0, cols))
        if index == 27:
            return v_block(z, 1 - xl, c_, None)
        if index < 36:
            direction, k = (index - 28) // 4, (index - 28) % 4
            return x_forward(origin(direction, k + 1), 1 - xl, c_, direction, k, client)
        if index >= 44:
            direction, k = (index - 44) // 4, (index - 44) % 4
            return block(4, origin(direction, k + 1), c_, k, direction, client)
        direction, k = (index - 36) // 4, (index - 36) % 4
        return o_block(origin(direction, k + 1), xl, c_, o_span(3, k, direction, client))

    def d_group(index):
        if index in (1, 27):
            return 1
        if 2 <= index < 26 and (index - 2) % 3 == 0:
            return 2 + (index - 2) // 3 % 4
        if 28 <= index < 36:
            return 2 + (index - 28) % 4
        if index >= 44:
            return 2 + (index - 44) % 4
        return 0

    def d_copy(index, client):
        dst = d_refs(index, core, client)
        src = (ot_own, vt_own)[index] if index < 2 else dst
        return remote(src, dst, ds_, dr, d_group(index), dev(z, xl, 1 - core))

    def d_arrivals(group):
        units = {0: 16, 1: 2, 5: 2}.get(group, 4)
        ref = wot.at[pl.ds(0, units * cols), :]
        return remote(ref, ref, ds_, dr, group, dev(z, xl, 1 - core))

    def all_sent(sends, ref):
        remote(ref, ref, sends, dr, 0, dev(z, xl, 1 - core)).wait_send()

    def lent_copy():
        return remote(ot_own.at[pl.ds(0, lent), :], held.at[z], hs, hr, 0, outer)

    def lent_arrival():
        return remote(held.at[z], held.at[z], hs, hr, 0, outer)

    def back_copy(direction, k):
        zo = origin(direction, k + 1)
        span = o_span(3, k, direction, True)
        return remote(
            held.at[zo, pl.ds(*span), :], o_block(zo, 1 - xl, core, span), hs, hr, 1 + direction * 4 + k, outer
        )

    def back_arrival(direction, k):
        ref = o_block(origin(direction, k + 1), xl, core, o_span(3, k, direction, True))
        return remote(ref, ref, hs, hr, 1 + direction * 4 + k, outer)

    def value_pair(z_, x_):
        span = pl.ds(pl.multiple_of((z_ * 4 + x_ * 2) * cols, 2 * cols), 2 * cols)
        left = normed[:, span]
        for n in range(0, kv, 256):
            va_sum[:, n : n + 256] += lax.dot_general(
                left, wvt[n : n + 256, span], (((1,), (1,)), ((), ())), preferred_element_type=jnp.float32
            )

    def pairs_of(k, client):
        d_arrivals(2 + k).wait_recv()
        for direction in (0, 1):
            if 0 <= k < 3 or direction == 1:
                value_pair(origin(direction, k + 1), 0)
                value_pair(origin(direction, k + 1), 1)

    def begin(client):
        x_copy(0, client).start()
        x_copy(1, client).start()
        if client:
            lent_copy().start()
        for item in (0, 1) if client else (0,):
            for direction in (0, 1):
                z_copy(direction, 0, item, client).start()
        d_copy(0, client).start()
        d_copy(1, client).start()

    def z_step(direction, k, item, client):
        z_arrival(direction, k, item, client).wait_recv()
        if k < 3:
            z_copy(direction, k + 1, item, client).start()
        if item == 0:
            x_copy(2 + direction * 4 + k, client).start()
        if item == 3:
            back_copy(direction, k).start()
        elif item == 4:
            d_copy(44 + direction * 4 + k, client).start()
        else:
            d_copy(2 + direction * 12 + k * 3 + item, client).start()

    def x_step(k, client):
        for direction in (0, 1):
            x_arrival(2 + direction * 4 + k, client).wait_recv()
            d_copy(28 + direction * 4 + k, client).start()

    def last_waits(client):
        pairs_of(3, client)
        d_arrivals(0).wait_recv()

    def gather_client():
        x_arrival(0, True).wait_recv()
        for direction in (0, 1):
            z_copy(direction, 0, 2, True).start()
        d_copy(26, True).start()
        for k in range(4):
            for item in (0, 1):
                for direction in (0, 1):
                    z_step(direction, k, item, True)
            if k == 0:
                x_arrival(1, True).wait_recv()
                d_copy(27, True).start()
                for direction in (0, 1):
                    z_copy(direction, 0, 4, True).start()
            else:
                x_step(k - 1, True)
            for direction in (0, 1):
                back_arrival(direction, k).wait_recv()
                d_copy(36 + direction * 4 + k, True).start()
            for item in (2, 4):
                for direction in (0, 1):
                    z_step(direction, k, item, True)
            if k > 0:
                pairs_of(k - 2, True)
        pairs_of(2, True)
        x_step(3, True)
        last_waits(True)

    def gather_helper():
        lent_arrival().wait_recv()
        for direction in (0, 1):
            z_copy(direction, 0, 3, False).start()
        x_arrival(0, False).wait_recv()
        d_copy(26, False).start()
        for k in range(4):
            if k == 3:
                for item in (1, 2):
                    for direction in (0, 1):
                        z_copy(direction, 0, item, False).start()
            for item in (0, 3):
                for direction in (0, 1):
                    z_step(direction, k, item, False)
        x_arrival(1, False).wait_recv()
        d_copy(27, False).start()
        for k in range(4):
            for item in (1, 2):
                for direction in (0, 1):
                    z_step(direction, k, item, False)
            x_step(k, False)
            pairs_of(k - 1, False)
        last_waits(False)

    half_of = SECTIONS // 2

    @pl.when(sec >= half_of)
    def _():
        begin(True)

    @pl.when(sec < half_of)
    def _():
        begin(False)

    own = pl.ds(pl.multiple_of(shard * cols, cols), cols)
    wvt[:, own] = vt_own[...]
    wot[own, :] = ot_own[...]

    def prepare(b, carry):
        rows = pl.ds(pl.multiple_of(b * ROWS, ROWS), ROWS)
        hidden = act[rows, :].astype(jnp.float32)
        inverse = lax.rsqrt(jnp.mean(hidden * hidden, axis=-1, keepdims=True) + EPSILON)
        rms[rows, :] = jnp.broadcast_to(inverse, (ROWS, 128))
        normed[rows, :] = (hidden * inverse * gain[...]).astype(jnp.bfloat16)
        return carry

    local[0].wait()
    lax.fori_loop(0, BLOCKS, prepare, 0)
    local[4].wait()

    @pl.when(sec == SECTIONS - 1)
    def _():
        def masked(b, carry):
            rows = pl.ds(pl.multiple_of(b * ROWS, ROWS), ROWS)
            row_at = lax.broadcasted_iota(jnp.int32, (ROWS, LEN), 0) + b * ROWS
            col_at = lax.broadcasted_iota(jnp.int32, (ROWS, LEN), 1)
            kept = jnp.where(row_at == col_at, mask[...].astype(jnp.float32), 0.0)
            column = jnp.sum(kept, axis=-1, keepdims=True)
            c_in[b] = (top[rows, :].astype(jnp.float32) * column).astype(jnp.bfloat16)
            return carry

        lax.fori_loop(0, BLOCKS, masked, 0)

    local[1].wait()
    local[2].wait()
    local[3].wait()

    @pl.when(sec == 0)
    def _():
        ahead(0).start()


    def lowered(b, carry):
        rows = pl.ds(pl.multiple_of(b * ROWS, ROWS), ROWS)
        store_low[rows, :] = store[rows, :].astype(jnp.bfloat16)
        return carry

    lax.fori_loop(0, store.shape[0] // ROWS, lowered, 0)
    va_sum[...] = jnp.zeros_like(va_sum)

    @pl.when(sec >= half_of)
    def _():
        gather_client()

    @pl.when(sec < half_of)
    def _():
        gather_helper()

    def value_path():
        va[...] = va_sum[...].astype(jnp.bfloat16)
        vlow[...] = lax.dot_general(
            va[...], vproj[...], (((1,), (1,)), ((), ())), preferred_element_type=jnp.float32
        )

    piece = width // PIECES

    def c_copy(b, n):
        span = pl.ds(n * piece, piece)
        group = [first <= n < last for first, last in GROUPS].index(True)
        return pltpu.make_async_remote_copy(
            src_ref=c_out.at[b, :, span], dst_ref=c_in.at[b, :, span], send_sem=cs.at[0], recv_sem=cr.at[b, group],
            device_id=(down, shard), device_id_type=MESH,
        )

    def arrived(b, group):
        first, last = GROUPS[group]
        ref = c_in.at[b, :, pl.ds(first * piece, (last - first) * piece)]
        pltpu.make_async_remote_copy(
            src_ref=ref, dst_ref=ref, send_sem=cs.at[0], recv_sem=cr.at[b, group],
            device_id=(up, shard), device_id_type=MESH,
        ).wait_recv()

    half_rows = gproj.shape[0] // 2

    def features(source, right, values, own_feat):
        low = lax.dot_general(
            source[...].reshape(LEN, width), right[...], (((1,), (1,)), ((), ())), preferred_element_type=jnp.float32
        )
        feat[...] = lax.dot_general(
            low, values[...], (((0,), (0,)), ((), ())),
            precision=lax.Precision.HIGHEST, preferred_element_type=jnp.float32,
        )
        even = feat[pl.ds(0, half_rows, stride=2), :]
        odd = feat[pl.ds(1, half_rows, stride=2), :]
        packed = jnp.concatenate([even, odd], axis=1).astype(jnp.bfloat16)
        own_feat[...] = packed

    @pl.when(sec < SECTIONS - 1)
    def _():
        value_path()

    def stage(b, top_layer, eager, sending):
        rows = pl.ds(pl.multiple_of(b * ROWS, ROWS), ROWS)
        if eager:
            grad_value = jnp.zeros((ROWS, kv), jnp.float32)
            for group, (first, last) in enumerate(GROUPS):
                arrived(b, group)
                span = slice(first * piece, last * piece)
                grad_value += jnp.dot(c_in[b, :, span], wot[span, :], preferred_element_type=jnp.float32)
        else:
            if not top_layer:
                for group in range(len(GROUPS)):
                    arrived(b, group)
            grad_value = jnp.dot(c_in[b], wot[...], preferred_element_type=jnp.float32)
        grad_value = grad_value.astype(jnp.bfloat16)
        inverse = rms[rows, :][:, :1]
        total = jnp.sum(grad_value.astype(jnp.float32) * va_sum[rows, :], axis=-1, keepdims=True)
        back = (inverse * inverse) * (total / width)
        for n in range(PIECES):
            span = slice(n * piece, (n + 1) * piece)
            part = gain[:, span] * jnp.dot(grad_value, wvt[:, span], preferred_element_type=jnp.float32)
            hidden = act[rows, span].astype(jnp.float32)
            grad_input = inverse * part - hidden * back
            c_out[b, :, span] = (c_in[b, :, span].astype(jnp.float32) + grad_input).astype(jnp.bfloat16)
            if sending:
                c_copy(b, n).start()

    def stages(top_layer, sending):
        def one(b, carry):
            stage(b, top_layer, False, sending)
            return carry

        if not top_layer:
            stage(0, False, True, sending)
        lax.fori_loop(0 if top_layer else 1, BLOCKS, one, 0)

    def rows_of(count):
        return wot.at[pl.ds(0, count), :]

    def settle():
        wide = 7 * cols
        moved = side * cols // kv

        @pl.when(sec >= half_of)
        def _():
            all_sent(zs, rows_of(2 * wide + 7 * (cols - lent) + 7 * moved))
            all_sent(hs, rows_of(lent))
            all_sent(xs, rows_of(2 * cols + wide - 7 * moved))

        @pl.when(sec < half_of)
        def _():
            all_sent(zs, rows_of(3 * wide + 7 * lent))
            all_sent(hs, rows_of(7 * lent))
            all_sent(xs, rows_of(2 * cols + wide))

        all_sent(ds_, rows_of(4 * wide + 4 * cols))

    @pl.when(sec < SECTIONS - 1)
    def _():
        settle()

    @pl.when(sec == 0)
    def _():
        ahead(1).start()

    @pl.when((sec > 1) & (sec < SECTIONS - 1))
    def _():
        stages(False, True)

    @pl.when(sec == SECTIONS - 1)
    def _():
        stages(True, True)

    def n_copy(p):
        return pltpu.make_async_remote_copy(
            src_ref=feat_in, dst_ref=feats.at[shard], send_sem=ns.at[0], recv_sem=fr.at[p],
            device_id=(down, dev((z + p // 2) % NZ, (xl + p) % 2, core)[1]), device_id_type=MESH,
        )

    near = (0, 1, 7, 2, 6, 3, 5, 4)
    order = [2 * dz + dx for dz in near for dx in (0, 1)]

    @pl.when(sec == 1)
    def _():
        stages(False, False)
        ahead(0).wait_recv()
        ahead(1).wait_recv()
        features(c_out, gproj_in, vlow_in, feat_in)
        for p in reversed(order):
            n_copy(p).start()

    @pl.when(sec == SECTIONS - 1)
    def _():
        value_path()

    @pl.when(sec > 0)
    def _():
        features(c_in, gproj, vlow, feat_own)
        feats[shard] = feat_own[...]

    def slot(p, c_):
        return ((z + NZ - p // 2) % NZ) * 4 + ((xl + p) % 2) * 2 + c_

    def f_copy(p):
        return pltpu.make_async_remote_copy(
            src_ref=feat_own, dst_ref=feats.at[shard], send_sem=fs.at[0], recv_sem=fr.at[p],
            device_id=dev((z + p // 2) % NZ, (xl + p) % 2, core), device_id_type=MESH,
        )

    def f_arrival(p):
        ref = feats.at[slot(p, core)]
        return pltpu.make_async_remote_copy(
            src_ref=ref, dst_ref=ref, send_sem=fs.at[0], recv_sem=fr.at[p],
            device_id=dev((z + NZ - p // 2) % NZ, (xl + p) % 2, core), device_id_type=MESH,
        )

    def g_copy(p):
        ref = feats.at[slot(p, core)]
        return pltpu.make_async_remote_copy(
            src_ref=ref, dst_ref=ref, send_sem=gs.at[0], recv_sem=gr.at[0],
            device_id=dev(z, xl, 1 - core), device_id_type=MESH,
        )

    def g_arrivals():
        ref = feats.at[pl.ds(0, 2 * NZ)]
        return pltpu.make_async_remote_copy(
            src_ref=ref, dst_ref=ref, send_sem=gs.at[0], recv_sem=gr.at[0],
            device_id=dev(z, xl, 1 - core), device_id_type=MESH,
        )

    @pl.when(sec > 0)
    def _():
        for p in reversed(order[1:]):
            f_copy(p).start()
        g_copy(0).start()
        for p in order[1:]:
            f_arrival(p).wait_recv()
            g_copy(p).start()

    @pl.when(sec == 0)
    def _():
        for p in order:
            f_arrival(p).wait_recv()
            g_copy(p).start()

    g_arrivals().wait_recv()
    gens = feats.shape[0]
    for q in range(gens):
        feat_rows[q * half_rows : (q + 1) * half_rows, :] = feats[q].astype(jnp.float32)
    for i in range(half_rows):
        feat_all[:, i * 128 : (i + 1) * 128] = feat_rows[pl.ds(i, gens, stride=half_rows), :].astype(jnp.bfloat16)
    scores = lax.dot_general(
        feat_all[...], store_low[...], (((1,), (1,)), ((), ())), preferred_element_type=jnp.float32
    )
    gens_each = gens // SECTIONS
    for n in range(SECTIONS):
        part_out[n] = scores[n * gens_each : (n + 1) * gens_each, :]

    def p_copy(d):
        return pltpu.make_async_remote_copy(
            src_ref=part_out.at[(sec + d) % SECTIONS], dst_ref=part_in.at[d], send_sem=ps.at[0], recv_sem=pr.at[0],
            device_id=((sec + d) % SECTIONS, shard), device_id_type=MESH,
        )

    def p_arrivals():
        ref = part_in.at[pl.ds(1, SECTIONS - 1)]
        return pltpu.make_async_remote_copy(
            src_ref=ref, dst_ref=ref, send_sem=ps.at[0], recv_sem=pr.at[0],
            device_id=(down, shard), device_id_type=MESH,
        )

    for d in range(1, SECTIONS):
        p_copy(d).start()
    all_sent(gs, feats.at[pl.ds(0, 2 * NZ)])

    @pl.when(sec == 0)
    def _():
        ahead(0).wait_send()
        ahead(1).wait_send()

    @pl.when(sec == 1)
    def _():
        all_sent(ns, feats.at[pl.ds(0, 2 * NZ)])

    @pl.when(sec > 0)
    def _():
        all_sent(fs, feats.at[pl.ds(0, 2 * NZ - 1)])

    @pl.when(sec > 1)
    def _():
        all_sent(cs, c_out)

    @pl.when(sec == SECTIONS - 1)
    def _():
        settle()

    part_in[0] = part_out[sec]
    p_arrivals().wait_send()
    p_arrivals().wait_recv()
    out[...] = part_in[...]


def chain(act, top, mask, gain, v_own, o_own, vproj, gproj, store):
    tokens, width = act.shape
    kv = v_own.shape[1]
    proj = vproj.shape[0]
    examples = store.shape[0]
    gens = NZ * 4
    vmem = pl.BlockSpec(memory_space=pltpu.VMEM)
    hbm = pl.BlockSpec(memory_space=pltpu.HBM)
    dma = pltpu.SemaphoreType.DMA
    bf16, f32 = jnp.bfloat16, jnp.float32
    return pl.pallas_call(
        chain_kernel,
        out_shape=jax.ShapeDtypeStruct((SECTIONS, gens // SECTIONS, examples), f32),
        in_specs=[hbm, hbm, vmem, vmem] + [hbm] * 5,
        out_specs=vmem,
        scratch_shapes=[
            pltpu.VMEM(act.shape, bf16),
            pltpu.VMEM(top.shape, bf16),
            pltpu.VMEM(vproj.shape, bf16),
            pltpu.VMEM(gproj.shape, bf16),
            pltpu.VMEM(store.shape, f32),
            pltpu.VMEM(v_own.shape, bf16),
            pltpu.VMEM(o_own.shape, bf16),
            pltpu.VMEM(v_own.shape[::-1], bf16),
            pltpu.VMEM(o_own.shape[::-1], bf16),
            pltpu.VMEM(store.shape, bf16),
            pltpu.VMEM((kv, width), bf16),
            pltpu.VMEM((width, kv), bf16),
            pltpu.VMEM((NZ, v_own.shape[0] * 3 // 4, kv), bf16),
            pltpu.VMEM((tokens, width), bf16),
            pltpu.VMEM((tokens, 128), f32),
            pltpu.VMEM((BLOCKS, ROWS, width), bf16),
            pltpu.VMEM((BLOCKS, ROWS, width), bf16),
            pltpu.VMEM((tokens, kv), f32),
            pltpu.VMEM((tokens, kv), bf16),
            pltpu.VMEM((tokens, proj), f32),
            pltpu.VMEM((proj, proj), f32),
            pltpu.VMEM((proj // 2, 2 * proj), bf16),
            pltpu.VMEM(gproj.shape, bf16),
            pltpu.VMEM((tokens, proj), f32),
            pltpu.VMEM((proj // 2, 2 * proj), bf16),
            pltpu.VMEM((gens, proj // 2, 2 * proj), bf16),
            pltpu.VMEM((gens * proj // 2, 2 * proj), f32),
            pltpu.VMEM((gens, proj * proj), bf16),
            pltpu.VMEM((SECTIONS, gens // SECTIONS, examples), f32),
            pltpu.VMEM((SECTIONS, gens // SECTIONS, examples), f32),
            dma((7,)),
            dma((1,)), dma((2, 4, 5)), dma((1,)), dma((10,)), dma((1,)), dma((6,)), dma((1,)), dma((9,)),
            dma((1,)), dma((BLOCKS, len(GROUPS))),
            dma((1,)), dma((2 * NZ,)), dma((1,)), dma((1,)), dma((1,)), dma((1,)), dma((2,)), dma((2,)), dma((1,)),
        ],
        compiler_params=pltpu.CompilerParams(
            collective_id=0, has_side_effects=True, vmem_limit_bytes=60 * 1024 * 1024
        ),
        cost_estimate=pl.CostEstimate(flops=3 * 10**9, bytes_accessed=4 * 10**6, transcendentals=0),
    )(act, top, mask, gain, v_own, o_own, vproj, gproj, store)


def per_device(
    activations, top_grad, loss_mask, norm_gain, value_weight, output_weight, value_proj, grad_proj, store
):
    parts = chain(
        activations[0], top_grad, loss_mask.reshape(1, -1), norm_gain, value_weight[0], output_weight[0],
        value_proj[0].T, grad_proj[0].T, store[0],
    )
    return parts.sum(axis=0)


def solution(mesh):
    placed = (
        P("section", "shard", None),
        P("shard", None),
        P("shard"),
        P("section", None),
        P("section", "shard", None),
        P("section", None, "shard"),
        P("section", None, None),
        P("section", None, None),
        P("section", "shard", None),
    )
    return jax.shard_map(
        per_device, mesh=mesh, in_specs=placed, out_specs=P("section", "shard"), check_vma=False
    )
```

```python
import jax
import jax.numpy as jnp
from jax import lax
from jax.experimental import pallas as pl
from jax.experimental.pallas import tpu as pltpu
from jax.sharding import PartitionSpec as P

LEN = 96
EPSILON = 1e-05
MESH = pl.DeviceIdType.MESH
NZ = 8
SECTIONS = 8
ROWS = 16
BLOCKS = LEN // ROWS
PIECES = 4
GROUPS = ((0, 2), (2, 3), (3, 4))


def chain_kernel(
    act_hbm, top_hbm, mask, gain, v_hbm, o_hbm, vproj_hbm, gproj_hbm, store_hbm,
    out,
    act, top, vproj, gproj, store, v_raw, o_raw, vt_own, ot_own, store_low,
    wvt, wot, held, normed, rms, c_in, c_out, va_sum, va, vlow,
    feat, feat_own, gproj_in, vlow_in, feat_in, feats, feat_rows, feat_all, part_out, part_in,
    ls, zs, zr, xs, xr, ds_, dr, hs, hr, cs, cr, fs, fr, gs, gr, ps, pr, es, er, ns,
):
    sec = lax.axis_index("section")
    shard = lax.axis_index("shard")
    z = shard // 4
    xl = (shard // 2) % 2
    core = shard % 2
    width = act.shape[1]
    kv = wot.shape[1]
    cols = vt_own.shape[1]

    def dev(z_, x_, c_):
        return (sec, z_ * 4 + x_ * 2 + c_)

    z_next = (z + 1) % NZ
    z_prev = (z + NZ - 1) % NZ
    up = (sec + 1) % SECTIONS
    down = (sec + SECTIONS - 1) % SECTIONS
    own_v = pltpu.make_async_copy(v_hbm, v_raw, ls.at[0])
    own_o = pltpu.make_async_copy(o_hbm, o_raw, ls.at[1])
    own_v.start()
    own_o.start()
    barrier = pltpu.get_barrier_semaphore()
    peers = [dev((z + p // 2) % NZ, (xl + p) % 2, core) for p in range(1, 2 * NZ)]
    outer = ((sec + SECTIONS // 2) % SECTIONS, z * 4 + (1 - xl) * 2 + core)
    peers.append(outer)
    peers.append(dev(z, xl, 1 - core))
    peers.extend([((sec + d) % SECTIONS, shard) for d in range(1, SECTIONS)])
    for peer in peers:
        pl.semaphore_signal(barrier, inc=1, device_id=peer, device_id_type=MESH)

    @pl.when(sec == 0)
    def _():
        for p in range(1, 2 * NZ):
            _, place = dev((z + p // 2) % NZ, (xl + p) % 2, core)
            pl.semaphore_signal(barrier, inc=1, device_id=(1, place), device_id_type=MESH)

    local = [
        pltpu.make_async_copy(source, target, ls.at[2 + n])
        for n, (source, target) in enumerate(
            ((act_hbm, act), (gproj_hbm, gproj), (vproj_hbm, vproj), (store_hbm, store), (top_hbm, top))
        )
    ]
    for copy in local:
        copy.start()
    own_o.wait()
    ot_own[...] = o_raw[...].T
    own_v.wait()
    vt_own[...] = v_raw[...].T

    @pl.when(sec == 1)
    def _():
        pl.semaphore_wait(barrier, len(peers) + 2 * NZ - 1)

    @pl.when(sec != 1)
    def _():
        pl.semaphore_wait(barrier, len(peers))

    def ahead(n):
        return pltpu.make_async_remote_copy(
            src_ref=(gproj, vlow)[n], dst_ref=(gproj_in, vlow_in)[n], send_sem=es.at[n], recv_sem=er.at[n],
            device_id=(up, shard), device_id_type=MESH,
        )


    def v_block(z_, x_, c_, half):
        first = pl.multiple_of((z_ * 4 + x_ * 2 + c_) * cols, cols)
        if half is None:
            return wvt.at[:, pl.ds(first, cols)]
        return wvt.at[pl.ds(half * (kv // 2), kv // 2), pl.ds(first, cols)]

    def v_rows(z_, x_, c_, begin, size):
        first = pl.multiple_of((z_ * 4 + x_ * 2 + c_) * cols, cols)
        return wvt.at[pl.ds(begin, size), pl.ds(first, cols)]

    def o_block(z_, x_, c_, span):
        begin, size = span
        first = pl.multiple_of((z_ * 4 + x_ * 2 + c_) * cols + begin, 16)
        return wot.at[pl.ds(first, size), :]

    lent = cols * 3 // 4
    side = kv // 8

    def o_span(item, k, direction, client):
        begin, size = 0, cols
        if item == 3:
            size = lent
        if item == 1 and client:
            begin, size = lent, cols - lent
        if k == 3:
            size = size // 2
            begin += direction * size
        return begin, size

    def block(item, z_, c_, k, direction, client):
        if item == 0:
            return v_block(z_, xl, c_, None if k < 3 else direction)
        if item == 4:
            return v_rows(z_, 1 - xl, c_, *((0, side) if k < 3 else (direction * side // 2, side // 2)))
        span = o_span(item, k, direction, client)
        if item == 3:
            return held.at[z_, pl.ds(*span), :]
        return o_block(z_, xl if item == 1 else 1 - xl, c_, span)

    def origin(direction, hops):
        return (z + (NZ - hops if direction == 0 else hops)) % NZ

    def remote(src, dst, sends, recvs, index, peer):
        return pltpu.make_async_remote_copy(
            src_ref=src, dst_ref=dst, send_sem=sends.at[0], recv_sem=recvs.at[index],
            device_id=peer, device_id_type=MESH,
        )

    def z_copy(direction, k, item, client):
        dst = block(item, origin(direction, k), core, k, direction, client)
        src = dst
        if k == 0 and item == 0:
            src = vt_own
        if k == 0 and item == 1:
            src = ot_own.at[pl.ds(*o_span(1, 0, direction, client)), :]
        return remote(src, dst, zs, zr, (direction, k, item), dev(z_next if direction == 0 else z_prev, xl, core))

    def z_arrival(direction, k, item, client):
        ref = block(item, origin(direction, k + 1), core, k, direction, client)
        return remote(ref, ref, zs, zr, (direction, k, item), dev(z_prev if direction == 0 else z_next, xl, core))

    def x_forward(z_, x_, c_, direction, k, client):
        begin, end = (0, kv) if k < 3 else (direction * (kv // 2), (direction + 1) * (kv // 2))
        if client:
            begin = max(begin, side)
        return v_rows(z_, x_, c_, begin, end - begin)

    def x_refs(index, x_, client):
        if index == 0:
            return o_block(z, x_, core, (0, cols))
        if index == 1:
            return v_block(z, x_, core, None)
        direction, k = (index - 2) // 4, (index - 2) % 4
        return x_forward(origin(direction, k + 1), x_, core, direction, k, client)

    def x_copy(index, client):
        dst = x_refs(index, xl, client)
        return remote((ot_own, vt_own)[index] if index < 2 else dst, dst, xs, xr, index, dev(z, 1 - xl, core))

    def x_arrival(index, client):
        ref = x_refs(index, 1 - xl, client)
        return remote(ref, ref, xs, xr, index, dev(z, 1 - xl, core))

    def d_refs(index, c_, client):
        if index == 0:
            return o_block(z, xl, c_, (0, cols))
        if index == 1:
            return v_block(z, xl, c_, None)
        if index < 26:
            direction, k, item = (index - 2) // 12, (index - 2) // 3 % 4, (index - 2) % 3
            return block(item, origin(direction, k + 1), c_, k, direction, client)
        if index == 26:
            return o_block(z, 1 - xl, c_, (0, cols))
        if index == 27:
            return v_block(z, 1 - xl, c_, None)
        if index < 36:
            direction, k = (index - 28) // 4, (index - 28) % 4
            return x_forward(origin(direction, k + 1), 1 - xl, c_, direction, k, client)
        if index >= 44:
            direction, k = (index - 44) // 4, (index - 44) % 4
            return block(4, origin(direction, k + 1), c_, k, direction, client)
        direction, k = (index - 36) // 4, (index - 36) % 4
        return o_block(origin(direction, k + 1), xl, c_, o_span(3, k, direction, client))

    def d_group(index):
        if index in (1, 27):
            return 1
        if 2 <= index < 26 and (index - 2) % 3 == 0:
            return 2 + (index - 2) // 3 % 4
        if 28 <= index < 36:
            return 2 + (index - 28) % 4
        if index >= 44:
            return 2 + (index - 44) % 4
        return 0

    def d_copy(index, client):
        dst = d_refs(index, core, client)
        src = (ot_own, vt_own)[index] if index < 2 else dst
        return remote(src, dst, ds_, dr, d_group(index), dev(z, xl, 1 - core))

    def d_arrivals(group):
        units = {0: 16, 1: 2, 5: 2}.get(group, 4)
        ref = wot.at[pl.ds(0, units * cols), :]
        return remote(ref, ref, ds_, dr, group, dev(z, xl, 1 - core))

    def all_sent(sends, ref):
        remote(ref, ref, sends, dr, 0, dev(z, xl, 1 - core)).wait_send()

    def lent_copy():
        return remote(ot_own.at[pl.ds(0, lent), :], held.at[z], hs, hr, 0, outer)

    def lent_arrival():
        return remote(held.at[z], held.at[z], hs, hr, 0, outer)

    def back_copy(direction, k):
        zo = origin(direction, k + 1)
        span = o_span(3, k, direction, True)
        return remote(
            held.at[zo, pl.ds(*span), :], o_block(zo, 1 - xl, core, span), hs, hr, 1 + direction * 4 + k, outer
        )

    def back_arrival(direction, k):
        ref = o_block(origin(direction, k + 1), xl, core, o_span(3, k, direction, True))
        return remote(ref, ref, hs, hr, 1 + direction * 4 + k, outer)

    def value_pair(z_, x_):
        span = pl.ds(pl.multiple_of((z_ * 4 + x_ * 2) * cols, 2 * cols), 2 * cols)
        left = normed[:, span]
        for n in range(0, kv, 256):
            va_sum[:, n : n + 256] += lax.dot_general(
                left, wvt[n : n + 256, span], (((1,), (1,)), ((), ())), preferred_element_type=jnp.float32
            )

    def pairs_of(k, client):
        d_arrivals(2 + k).wait_recv()
        for direction in (0, 1):
            if 0 <= k < 3 or direction == 1:
                value_pair(origin(direction, k + 1), 0)
                value_pair(origin(direction, k + 1), 1)

    def begin(client):
        x_copy(0, client).start()
        x_copy(1, client).start()
        if client:
            lent_copy().start()
        for item in (0, 1) if client else (0,):
            for direction in (0, 1):
                z_copy(direction, 0, item, client).start()
        d_copy(0, client).start()
        d_copy(1, client).start()

    def z_step(direction, k, item, client):
        z_arrival(direction, k, item, client).wait_recv()
        if k < 3:
            z_copy(direction, k + 1, item, client).start()
        if item == 0:
            x_copy(2 + direction * 4 + k, client).start()
        if item == 3:
            back_copy(direction, k).start()
        elif item == 4:
            d_copy(44 + direction * 4 + k, client).start()
        else:
            d_copy(2 + direction * 12 + k * 3 + item, client).start()

    def x_step(k, client):
        for direction in (0, 1):
            x_arrival(2 + direction * 4 + k, client).wait_recv()
            d_copy(28 + direction * 4 + k, client).start()

    def last_waits(client):
        pairs_of(3, client)
        d_arrivals(0).wait_recv()

    def gather_client():
        x_arrival(0, True).wait_recv()
        for direction in (0, 1):
            z_copy(direction, 0, 2, True).start()
        d_copy(26, True).start()
        for k in range(4):
            for item in (0, 1):
                for direction in (0, 1):
                    z_step(direction, k, item, True)
            if k == 0:
                x_arrival(1, True).wait_recv()
                d_copy(27, True).start()
                for direction in (0, 1):
                    z_copy(direction, 0, 4, True).start()
            else:
                x_step(k - 1, True)
            for direction in (0, 1):
                back_arrival(direction, k).wait_recv()
                d_copy(36 + direction * 4 + k, True).start()
            for item in (2, 4):
                for direction in (0, 1):
                    z_step(direction, k, item, True)
            if k > 0:
                pairs_of(k - 2, True)
        pairs_of(2, True)
        x_step(3, True)
        last_waits(True)

    def gather_helper():
        lent_arrival().wait_recv()
        for direction in (0, 1):
            z_copy(direction, 0, 3, False).start()
        x_arrival(0, False).wait_recv()
        d_copy(26, False).start()
        for k in range(4):
            if k == 3:
                for item in (1, 2):
                    for direction in (0, 1):
                        z_copy(direction, 0, item, False).start()
            for item in (0, 3):
                for direction in (0, 1):
                    z_step(direction, k, item, False)
        x_arrival(1, False).wait_recv()
        d_copy(27, False).start()
        for k in range(4):
            for item in (1, 2):
                for direction in (0, 1):
                    z_step(direction, k, item, False)
            x_step(k, False)
            pairs_of(k - 1, False)
        last_waits(False)

    half_of = SECTIONS // 2

    @pl.when(sec >= half_of)
    def _():
        begin(True)

    @pl.when(sec < half_of)
    def _():
        begin(False)

    own = pl.ds(pl.multiple_of(shard * cols, cols), cols)
    wvt[:, own] = vt_own[...]
    wot[own, :] = ot_own[...]

    def prepare(b, carry):
        rows = pl.ds(pl.multiple_of(b * ROWS, ROWS), ROWS)
        hidden = act[rows, :].astype(jnp.float32)
        inverse = lax.rsqrt(jnp.mean(hidden * hidden, axis=-1, keepdims=True) + EPSILON)
        rms[rows, :] = jnp.broadcast_to(inverse, (ROWS, 128))
        normed[rows, :] = (hidden * inverse * gain[...]).astype(jnp.bfloat16)
        return carry

    local[0].wait()
    lax.fori_loop(0, BLOCKS, prepare, 0)
    local[4].wait()

    @pl.when(sec == SECTIONS - 1)
    def _():
        def masked(b, carry):
            rows = pl.ds(pl.multiple_of(b * ROWS, ROWS), ROWS)
            row_at = lax.broadcasted_iota(jnp.int32, (ROWS, LEN), 0) + b * ROWS
            col_at = lax.broadcasted_iota(jnp.int32, (ROWS, LEN), 1)
            kept = jnp.where(row_at == col_at, mask[...].astype(jnp.float32), 0.0)
            column = jnp.sum(kept, axis=-1, keepdims=True)
            c_in[b] = (top[rows, :].astype(jnp.float32) * column).astype(jnp.bfloat16)
            return carry

        lax.fori_loop(0, BLOCKS, masked, 0)

    local[1].wait()
    local[2].wait()
    local[3].wait()

    @pl.when(sec == 0)
    def _():
        ahead(0).start()


    def lowered(b, carry):
        rows = pl.ds(pl.multiple_of(b * ROWS, ROWS), ROWS)
        store_low[rows, :] = store[rows, :].astype(jnp.bfloat16)
        return carry

    lax.fori_loop(0, store.shape[0] // ROWS, lowered, 0)
    va_sum[...] = jnp.zeros_like(va_sum)

    @pl.when(sec >= half_of)
    def _():
        gather_client()

    @pl.when(sec < half_of)
    def _():
        gather_helper()

    def value_path():
        va[...] = va_sum[...].astype(jnp.bfloat16)
        vlow[...] = lax.dot_general(
            va[...], vproj[...], (((1,), (1,)), ((), ())), preferred_element_type=jnp.float32
        )

    piece = width // PIECES

    def c_copy(b, n):
        span = pl.ds(n * piece, piece)
        group = [first <= n < last for first, last in GROUPS].index(True)
        return pltpu.make_async_remote_copy(
            src_ref=c_out.at[b, :, span], dst_ref=c_in.at[b, :, span], send_sem=cs.at[0], recv_sem=cr.at[b, group],
            device_id=(down, shard), device_id_type=MESH,
        )

    def arrived(b, group):
        first, last = GROUPS[group]
        ref = c_in.at[b, :, pl.ds(first * piece, (last - first) * piece)]
        pltpu.make_async_remote_copy(
            src_ref=ref, dst_ref=ref, send_sem=cs.at[0], recv_sem=cr.at[b, group],
            device_id=(up, shard), device_id_type=MESH,
        ).wait_recv()

    half_rows = gproj.shape[0] // 2

    def features(source, right, values, own_feat):
        low = lax.dot_general(
            source[...].reshape(LEN, width), right[...], (((1,), (1,)), ((), ())), preferred_element_type=jnp.float32
        )
        feat[...] = lax.dot_general(
            low, values[...], (((0,), (0,)), ((), ())),
            precision=lax.Precision.HIGHEST, preferred_element_type=jnp.float32,
        )
        even = feat[pl.ds(0, half_rows, stride=2), :]
        odd = feat[pl.ds(1, half_rows, stride=2), :]
        packed = jnp.concatenate([even, odd], axis=1).astype(jnp.bfloat16)
        own_feat[...] = packed

    @pl.when(sec < SECTIONS - 1)
    def _():
        value_path()

    def stage(b, top_layer, eager, sending):
        rows = pl.ds(pl.multiple_of(b * ROWS, ROWS), ROWS)
        if eager:
            grad_value = jnp.zeros((ROWS, kv), jnp.float32)
            for group, (first, last) in enumerate(GROUPS):
                arrived(b, group)
                span = slice(first * piece, last * piece)
                grad_value += jnp.dot(c_in[b, :, span], wot[span, :], preferred_element_type=jnp.float32)
        else:
            if not top_layer:
                for group in range(len(GROUPS)):
                    arrived(b, group)
            grad_value = jnp.dot(c_in[b], wot[...], preferred_element_type=jnp.float32)
        grad_value = grad_value.astype(jnp.bfloat16)
        inverse = rms[rows, :][:, :1]
        total = jnp.sum(grad_value.astype(jnp.float32) * va_sum[rows, :], axis=-1, keepdims=True)
        back = (inverse * inverse) * (total / width)
        for n in range(PIECES):
            span = slice(n * piece, (n + 1) * piece)
            part = gain[:, span] * jnp.dot(grad_value, wvt[:, span], preferred_element_type=jnp.float32)
            hidden = act[rows, span].astype(jnp.float32)
            grad_input = inverse * part - hidden * back
            c_out[b, :, span] = (c_in[b, :, span].astype(jnp.float32) + grad_input).astype(jnp.bfloat16)
            if sending:
                c_copy(b, n).start()

    def stages(top_layer, sending):
        def one(b, carry):
            stage(b, top_layer, False, sending)
            return carry

        if not top_layer:
            stage(0, False, True, sending)
        lax.fori_loop(0 if top_layer else 1, BLOCKS, one, 0)

    def rows_of(count):
        return wot.at[pl.ds(0, count), :]

    def settle():
        wide = 7 * cols
        moved = side * cols // kv

        @pl.when(sec >= half_of)
        def _():
            all_sent(zs, rows_of(2 * wide + 7 * (cols - lent) + 7 * moved))
            all_sent(hs, rows_of(lent))
            all_sent(xs, rows_of(2 * cols + wide - 7 * moved))

        @pl.when(sec < half_of)
        def _():
            all_sent(zs, rows_of(3 * wide + 7 * lent))
            all_sent(hs, rows_of(7 * lent))
            all_sent(xs, rows_of(2 * cols + wide))

        all_sent(ds_, rows_of(4 * wide + 4 * cols))

    @pl.when(sec < SECTIONS - 1)
    def _():
        settle()

    @pl.when(sec == 0)
    def _():
        ahead(1).start()

    @pl.when((sec > 1) & (sec < SECTIONS - 1))
    def _():
        stages(False, True)

    @pl.when(sec == SECTIONS - 1)
    def _():
        stages(True, True)

    def n_copy(p):
        return pltpu.make_async_remote_copy(
            src_ref=feat_in, dst_ref=feats.at[shard], send_sem=ns.at[0], recv_sem=fr.at[p],
            device_id=(down, dev((z + p // 2) % NZ, (xl + p) % 2, core)[1]), device_id_type=MESH,
        )

    near = (0, 1, 7, 2, 6, 3, 5, 4)
    order = [2 * dz + dx for dz in near for dx in (0, 1)]

    @pl.when(sec == 1)
    def _():
        stages(False, False)
        ahead(0).wait_recv()
        ahead(1).wait_recv()
        features(c_out, gproj_in, vlow_in, feat_in)
        for p in reversed(order):
            n_copy(p).start()

    @pl.when(sec == SECTIONS - 1)
    def _():
        value_path()

    @pl.when(sec > 0)
    def _():
        features(c_in, gproj, vlow, feat_own)
        feats[shard] = feat_own[...]

    def slot(p, c_):
        return ((z + NZ - p // 2) % NZ) * 4 + ((xl + p) % 2) * 2 + c_

    def f_copy(p):
        return pltpu.make_async_remote_copy(
            src_ref=feat_own, dst_ref=feats.at[shard], send_sem=fs.at[0], recv_sem=fr.at[p],
            device_id=dev((z + p // 2) % NZ, (xl + p) % 2, core), device_id_type=MESH,
        )

    def f_arrival(p):
        ref = feats.at[slot(p, core)]
        return pltpu.make_async_remote_copy(
            src_ref=ref, dst_ref=ref, send_sem=fs.at[0], recv_sem=fr.at[p],
            device_id=dev((z + NZ - p // 2) % NZ, (xl + p) % 2, core), device_id_type=MESH,
        )

    def g_copy(p):
        ref = feats.at[slot(p, core)]
        return pltpu.make_async_remote_copy(
            src_ref=ref, dst_ref=ref, send_sem=gs.at[0], recv_sem=gr.at[0],
            device_id=dev(z, xl, 1 - core), device_id_type=MESH,
        )

    def g_arrivals():
        ref = feats.at[pl.ds(0, 2 * NZ)]
        return pltpu.make_async_remote_copy(
            src_ref=ref, dst_ref=ref, send_sem=gs.at[0], recv_sem=gr.at[0],
            device_id=dev(z, xl, 1 - core), device_id_type=MESH,
        )

    @pl.when(sec > 0)
    def _():
        for p in reversed(order[1:]):
            f_copy(p).start()
        g_copy(0).start()
        for p in order[1:]:
            f_arrival(p).wait_recv()
            g_copy(p).start()

    @pl.when(sec == 0)
    def _():
        for p in order:
            f_arrival(p).wait_recv()
            g_copy(p).start()

    g_arrivals().wait_recv()
    gens = feats.shape[0]
    for q in range(gens):
        feat_rows[q * half_rows : (q + 1) * half_rows, :] = feats[q].astype(jnp.float32)
    for i in range(half_rows):
        feat_all[:, i * 128 : (i + 1) * 128] = feat_rows[pl.ds(i, gens, stride=half_rows), :].astype(jnp.bfloat16)
    scores = lax.dot_general(
        feat_all[...], store_low[...], (((1,), (1,)), ((), ())), preferred_element_type=jnp.float32
    )
    gens_each = gens // SECTIONS
    for n in range(SECTIONS):
        part_out[n] = scores[n * gens_each : (n + 1) * gens_each, :]

    def p_copy(d):
        return pltpu.make_async_remote_copy(
            src_ref=part_out.at[(sec + d) % SECTIONS], dst_ref=part_in.at[d], send_sem=ps.at[0], recv_sem=pr.at[0],
            device_id=((sec + d) % SECTIONS, shard), device_id_type=MESH,
        )

    def p_arrivals():
        ref = part_in.at[pl.ds(1, SECTIONS - 1)]
        return pltpu.make_async_remote_copy(
            src_ref=ref, dst_ref=ref, send_sem=ps.at[0], recv_sem=pr.at[0],
            device_id=(down, shard), device_id_type=MESH,
        )

    for d in range(1, SECTIONS):
        p_copy(d).start()
    all_sent(gs, feats.at[pl.ds(0, 2 * NZ)])

    @pl.when(sec == 0)
    def _():
        ahead(0).wait_send()
        ahead(1).wait_send()

    @pl.when(sec == 1)
    def _():
        all_sent(ns, feats.at[pl.ds(0, 2 * NZ)])

    @pl.when(sec > 0)
    def _():
        all_sent(fs, feats.at[pl.ds(0, 2 * NZ - 1)])

    @pl.when(sec > 1)
    def _():
        all_sent(cs, c_out)

    @pl.when(sec == SECTIONS - 1)
    def _():
        settle()

    part_in[0] = part_out[sec]
    p_arrivals().wait_send()
    p_arrivals().wait_recv()
    out[...] = part_in[...]


def chain(act, top, mask, gain, v_own, o_own, vproj, gproj, store):
    tokens, width = act.shape
    kv = v_own.shape[1]
    proj = vproj.shape[0]
    examples = store.shape[0]
    gens = NZ * 4
    vmem = pl.BlockSpec(memory_space=pltpu.VMEM)
    hbm = pl.BlockSpec(memory_space=pltpu.HBM)
    dma = pltpu.SemaphoreType.DMA
    bf16, f32 = jnp.bfloat16, jnp.float32
    return pl.pallas_call(
        chain_kernel,
        out_shape=jax.ShapeDtypeStruct((SECTIONS, gens // SECTIONS, examples), f32),
        in_specs=[hbm, hbm, vmem, vmem] + [hbm] * 5,
        out_specs=vmem,
        scratch_shapes=[
            pltpu.VMEM(act.shape, bf16),
            pltpu.VMEM(top.shape, bf16),
            pltpu.VMEM(vproj.shape, bf16),
            pltpu.VMEM(gproj.shape, bf16),
            pltpu.VMEM(store.shape, f32),
            pltpu.VMEM(v_own.shape, bf16),
            pltpu.VMEM(o_own.shape, bf16),
            pltpu.VMEM(v_own.shape[::-1], bf16),
            pltpu.VMEM(o_own.shape[::-1], bf16),
            pltpu.VMEM(store.shape, bf16),
            pltpu.VMEM((kv, width), bf16),
            pltpu.VMEM((width, kv), bf16),
            pltpu.VMEM((NZ, v_own.shape[0] * 3 // 4, kv), bf16),
            pltpu.VMEM((tokens, width), bf16),
            pltpu.VMEM((tokens, 128), f32),
            pltpu.VMEM((BLOCKS, ROWS, width), bf16),
            pltpu.VMEM((BLOCKS, ROWS, width), bf16),
            pltpu.VMEM((tokens, kv), f32),
            pltpu.VMEM((tokens, kv), bf16),
            pltpu.VMEM((tokens, proj), f32),
            pltpu.VMEM((proj, proj), f32),
            pltpu.VMEM((proj // 2, 2 * proj), bf16),
            pltpu.VMEM(gproj.shape, bf16),
            pltpu.VMEM((tokens, proj), f32),
            pltpu.VMEM((proj // 2, 2 * proj), bf16),
            pltpu.VMEM((gens, proj // 2, 2 * proj), bf16),
            pltpu.VMEM((gens * proj // 2, 2 * proj), f32),
            pltpu.VMEM((gens, proj * proj), bf16),
            pltpu.VMEM((SECTIONS, gens // SECTIONS, examples), f32),
            pltpu.VMEM((SECTIONS, gens // SECTIONS, examples), f32),
            dma((7,)),
            dma((1,)), dma((2, 4, 5)), dma((1,)), dma((10,)), dma((1,)), dma((6,)), dma((1,)), dma((9,)),
            dma((1,)), dma((BLOCKS, len(GROUPS))),
            dma((1,)), dma((2 * NZ,)), dma((1,)), dma((1,)), dma((1,)), dma((1,)), dma((2,)), dma((2,)), dma((1,)),
        ],
        compiler_params=pltpu.CompilerParams(
            collective_id=0, has_side_effects=True, vmem_limit_bytes=60 * 1024 * 1024
        ),
        cost_estimate=pl.CostEstimate(flops=3 * 10**9, bytes_accessed=4 * 10**6, transcendentals=0),
    )(act, top, mask, gain, v_own, o_own, vproj, gproj, store)


def per_device(
    activations, top_grad, loss_mask, norm_gain, value_weight, output_weight, value_proj, grad_proj, store
):
    parts = chain(
        activations[0], top_grad, loss_mask.reshape(1, -1), norm_gain, value_weight[0], output_weight[0],
        value_proj[0].T, grad_proj[0].T, store[0],
    )
    return parts.sum(axis=0)


def solution(mesh):
    placed = (
        P("section", "shard", None),
        P("shard", None),
        P("shard"),
        P("section", None),
        P("section", "shard", None),
        P("section", None, "shard"),
        P("section", None, None),
        P("section", None, None),
        P("section", "shard", None),
    )
    return jax.shard_map(
        per_device, mesh=mesh, in_specs=placed, out_specs=P("section", "shard"), check_vma=False
    )
```
